256 devices in a mesh: section: 8 (over x, core), dp: 32 (over z, y).
Axes of the slice: x: 4, y: 4, z: 8, core: 2. Of those that a mesh axis runs over, the one named last changes fastest.
Arguments:
- hidden_in: bfloat16 [8, 2048, 2048], P(None, 'dp'), may hold values from -8 to 8
- norm_gain: bfloat16 [8, 2048], P('section'), may hold values from 0.099609375 to 1.8984375
- router_weight: bfloat16 [8, 2048, 60], P('section'), may hold values from -1 to 1
- expert_scale: bfloat16 [8, 60, 2048], P('section'), may hold values from 1 to 16
- mix_weight: bfloat16 [8, 2048, 2048], P('section'), may hold values from -0.125 to 0.125
- routes: int32 [8, 8, 2048, 4], P('section', None, 'dp'), may hold values from 0 to 59, as said below
Outputs:
- hidden_out: bfloat16 [8, 2048, 2048], P('section', 'dp')
- balance_loss: float32 [8], P('section')
The draws below stay inside these ranges and needn't reach their ends.
Inputs may be any that keep to these rules, and one draw needn't show every extreme that they name: `routes`: the 4 ids of a token in a layer are distinct.
All inputs are finite; a program needn't handle non-finite values.
Results may differ from the reference program's by a relative error of at most 0.01.
The reference program's roundings to bfloat16 on the way count: a program that leaves them out, or rounds other values in their place, can miss the bound.
Values may be sent and summed in bfloat16 or wider, within the bound.
No kernel may reach another device: no remote copies, remote signals or barrier semaphores. Data moves between devices by JAX's collectives and lax.ppermute only.
A program may use at most 64 MiB of HBM per device.

```python
import math
import jax
import jax.numpy as jnp
from jax import lax

D = 2048
E = 60
K = 4
M = 8
TOK_DEV = 64
TOK_MB = 2048
LAYERS = 8


def common_direction(key):
    signs = jax.random.randint(jax.random.fold_in(key, 7001), (D,), 0, 2)
    return signs.astype(jnp.float32) * 2.0 - 1.0


def draw_hidden_in(key, part):
    direction = common_direction(key)
    noise_key = jax.random.fold_in(key, 11)
    noise = jnp.clip(jax.random.normal(noise_key, (M, TOK_MB, D), jnp.float32), -6.0, 6.0)
    strength = jnp.ones((TOK_MB,), jnp.float32)
    values = noise + strength[None, :, None] * direction[None, None, :]
    return values.astype(jnp.bfloat16)


def draw_router_weight(key, part):
    direction = common_direction(key)
    noise = jnp.clip(jax.random.normal(jax.random.fold_in(key, 12), (LAYERS, D, E), jnp.float32), -6.0, 6.0)
    noise = noise / jnp.sqrt(jnp.float32(D))
    tilt = 2.0 * jnp.arange(E).astype(jnp.float32) / jnp.float32(E - 1) - 1.0
    lean = 4.0 * tilt[None, None, :] * direction[None, :, None] / jnp.float32(D)
    return (noise + lean).astype(jnp.bfloat16)


def draw_routes(key, part):
    shard_count = TOK_MB // TOK_DEV
    shard = jnp.arange(TOK_MB, dtype=jnp.int32) // TOK_DEV
    target = shard * (E - 1) // max(shard_count - 1, 1)
    expert_ids = jnp.arange(E, dtype=jnp.int32)
    distance = jnp.abs(expert_ids[None, :] - target[:, None])
    noise = jax.random.randint(jax.random.fold_in(key, 13), (LAYERS, M, TOK_MB, E), 0, 40)
    scores = (noise - distance[None, None, :, :]) * 64 + expert_ids[None, None, None, :]
    picked = lax.top_k(scores, K)[1]
    return picked.astype(jnp.int32)


def level_of(stream_key, dims, cuts, low, high):
    level, own = 1.0, jax.random.fold_in(stream_key, 6)
    for axis_at, shards_of in cuts:
        steps = jnp.exp(jax.random.uniform(jax.random.fold_in(own, axis_at), (shards_of,), jnp.float32, low / len(cuts), high / len(cuts)))
        level = level * jnp.repeat(steps, dims[axis_at] // shards_of).reshape([-1 if axis == axis_at else 1 for axis in range(len(dims))])
    return level


def bell_draw(key, shape, spread, most, shards=(), kind=jnp.bfloat16):
    gain = level_of(key, shape, shards, -0.22, 0.18) if shards else 1.0
    values = jax.random.normal(key, shape, jnp.float32) * spread * gain
    return jnp.minimum(jnp.maximum(values, -most), most).astype(kind)


def setup_inputs(seed: int = 0) -> dict:
    keys = jax.random.split(jax.random.key(seed), 7)
    return {
        "hidden_in": draw_hidden_in(jax.random.fold_in(keys[6], 71), 0),
        "norm_gain": jnp.clip(1.0 + 0.18 * jax.random.normal(keys[1], (LAYERS, D), jnp.float32), 0.099609375, 1.8984375).astype(jnp.bfloat16),
        "router_weight": draw_router_weight(jax.random.fold_in(keys[6], 71), 0),
        "expert_scale": jnp.clip(jnp.exp(math.log(16.0) - 2.7725887 * jax.random.uniform(keys[3], (LAYERS, E, D), jnp.float32) ** level_of(keys[3], (LAYERS, E, D), ((0, 8),), -0.2, 0.2)), 1.0, 16.0).astype(jnp.bfloat16),
        "mix_weight": bell_draw(keys[4], (LAYERS, D, D), D ** -0.5, 0.125, ((0, 8),)),
        "routes": draw_routes(jax.random.fold_in(keys[6], 71), 0),
    }


def router_layer(hidden_rows, gain_row, w_router, scale_table, w_mix, chosen_ids):
    state_wide = hidden_rows.astype(jnp.float32)
    mean_square = lax.optimization_barrier(jnp.mean(state_wide * state_wide, axis=-1, keepdims=True))
    normed = state_wide * lax.rsqrt(mean_square + 1e-06) * gain_row.astype(jnp.float32)
    logits = jnp.dot(normed.astype(jnp.bfloat16), w_router, preferred_element_type=jnp.float32)
    exponent = jnp.exp(logits)
    probabilities = exponent / lax.optimization_barrier(jnp.sum(exponent, axis=-1, keepdims=True))
    expert_ids = jnp.arange(w_router.shape[1], dtype=jnp.int32)
    onehot = lax.optimization_barrier(jnp.sum((chosen_ids[:, :, None] == expert_ids[None, None, :]).astype(jnp.float32), axis=1))
    gate_values = (probabilities * onehot).astype(jnp.bfloat16)
    channel_scale = jnp.dot(gate_values, scale_table, preferred_element_type=jnp.float32)
    mixed_rows = (normed * channel_scale).astype(jnp.bfloat16)
    update = jnp.dot(mixed_rows, w_mix, preferred_element_type=jnp.float32)
    updated = (state_wide + update).astype(jnp.bfloat16)
    return (updated, lax.optimization_barrier(jnp.sum(onehot, axis=0)), lax.optimization_barrier(jnp.sum(probabilities, axis=0)))

def reference(hidden_in, norm_gain, router_weight, expert_scale, mix_weight, routes):
    row_total = M * TOK_MB
    hidden_rows = hidden_in.reshape(row_total, D)
    losses = []
    for layer_index in range(LAYERS):
        chosen_ids = routes[layer_index].reshape(row_total, K)
        hidden_rows, counts, prob_sums = router_layer(hidden_rows, norm_gain[layer_index], router_weight[layer_index], expert_scale[layer_index], mix_weight[layer_index], chosen_ids)
        fractions = counts / jnp.float32(row_total * K)
        mean_probs = prob_sums / jnp.float32(row_total)
        losses.append(jnp.float32(E) * jnp.sum(fractions * mean_probs))
    return (hidden_rows.reshape(M, TOK_MB, D), jnp.stack(losses).astype(jnp.float32))
```

```python
import functools

import jax
import jax.numpy as jnp
from jax import lax
from jax.experimental import pallas as pl
from jax.experimental.pallas import tpu as pltpu
from jax.sharding import Mesh
from jax.sharding import PartitionSpec as P

SEC = ("x", "c")
CHIPS = 4
CHUNKS = 4
STEPS = 12
COLS = 256
WIDE = 512
VMEM_LIMIT = 12 * 1024 * 1024


def front(rows, load_x, load_gain, load_router, load_scale, ids, nrm, nbf, mixed):
    width = nrm.shape[1]
    acc = None
    for c in range(0, width, COLS):
        xs = load_x(c, COLS).astype(jnp.float32)
        acc = xs * xs if acc is None else acc + xs * xs
    mean_square = jnp.sum(acc, axis=-1, keepdims=True) * jnp.float32(1.0 / width)
    inv = lax.rsqrt(mean_square + 1e-06)
    for c in range(0, width, COLS):
        xs = load_x(c, COLS).astype(jnp.float32)
        normed = xs * inv * load_gain(c, COLS).astype(jnp.float32)
        nrm[0:rows, c : c + COLS] = normed
        nbf[0:rows, c : c + COLS] = normed.astype(jnp.bfloat16)
    logits = lax.dot_general(
        load_router(),
        nbf[0:rows, :],
        (((1,), (1,)), ((), ())),
        preferred_element_type=jnp.float32,
    )
    exponent = jnp.exp(logits)
    probs = exponent / jnp.sum(exponent, axis=0, keepdims=True)
    expert = lax.broadcasted_iota(jnp.int32, probs.shape, 0)
    hit = ids[0:1, :] == expert
    for k in range(1, ids.shape[0]):
        hit = hit | (ids[k : k + 1, :] == expert)
    chosen = jnp.where(hit, 1.0, 0.0).astype(jnp.float32)
    gates = jnp.transpose(probs * chosen).astype(jnp.bfloat16)
    for c in range(0, width, COLS):
        channel = jnp.dot(gates, load_scale(c, COLS), preferred_element_type=jnp.float32)
        mixed[0:rows, c : c + COLS] = (nrm[0:rows, c : c + COLS] * channel).astype(jnp.bfloat16)
    return (
        jnp.sum(probs, axis=1, keepdims=True),
        jnp.sum(chosen, axis=1, keepdims=True),
    )


def mix_block(rows, cur, mixed, w, n):
    update = jnp.dot(
        mixed[0:rows, :], w[:, n : n + WIDE], preferred_element_type=jnp.float32
    )
    cur[0:rows, n : n + WIDE] = (cur[0:rows, n : n + WIDE].astype(jnp.float32) + update).astype(
        jnp.bfloat16
    )


def add_stats(stats, lane, sums, counts):
    at = lax.broadcasted_iota(jnp.int32, stats.shape, 1)
    stats[...] += jnp.where(at == lane, sums, 0.0) + jnp.where(at == lane + 1, counts, 0.0)


def relay_layer(r, cur, sems=None):
    rows = cur.shape[0]
    sums, counts = front(
        rows,
        lambda c, n: cur[0:rows, c : c + n],
        lambda c, n: r["gain"][:, c : c + n],
        lambda: r["router"][...],
        lambda c, n: r["scale"][:, c : c + n],
        r["relay_ids"],
        r["nrm"],
        r["nbf"],
        r["mixed"],
    )
    for i, n in enumerate(range(0, cur.shape[1], WIDE)):
        if sems is not None:
            pltpu.make_async_copy(
                r["w_hbm"].at[:, pl.ds(n, WIDE)], r["w"].at[:, pl.ds(n, WIDE)], sems.at[i]
            ).wait()
        mix_block(rows, cur, r["mixed"], r["w"], n)
    return sums, counts


def step_kernel(t, names_in, names_out, names_scratch, *refs):
    r = dict(zip(names_in + names_out + names_scratch, refs))
    chip, core = lax.axis_index("x"), lax.axis_index("c")
    if "stats_in" in r:
        r["stats"][...] = r["stats_in"][...]
    else:
        r["stats"][...] = jnp.zeros_like(r["stats"])

    def pair_ids(ids, chunk):
        return jnp.concatenate([ids[2 * chunk], ids[2 * chunk + 1]], axis=1)

    if t == 0:
        width = r["w"].shape[1]
        first = (chip == 0) & (core == 0)

        @pl.when(first)
        def _():
            for b in range(2):
                pltpu.make_async_copy(
                    r["hidden"].at[b], r["sendR"].at[pl.ds(64 * b, 64)], r["xsem"].at[b]
                ).start()

        for i, n in enumerate(range(0, width, WIDE)):
            pltpu.make_async_copy(
                r["w_hbm"].at[:, pl.ds(n, WIDE)], r["w"].at[:, pl.ds(n, WIDE)], r["wsem"].at[i]
            ).start()

        @pl.when(first)
        def _():
            for b in range(2):
                pltpu.make_async_copy(
                    r["hidden"].at[b], r["sendR"].at[pl.ds(64 * b, 64)], r["xsem"].at[b]
                ).wait()
            r["relay_ids"] = pair_ids(r["ids"], 0)
            sums, counts = relay_layer(r, r["sendR"], r["wsem"])
            add_stats(r["stats"], 0, sums, counts)

        @pl.when(jnp.logical_not(first))
        def _():
            r["small"][0:60, :] = r["router"][...]
            r["small"][64:124, :] = r["scale"][...]
            r["small"][128:129, :] = r["gain"][...]
            for i, n in enumerate(range(0, width, WIDE)):
                pltpu.make_async_copy(
                    r["w_hbm"].at[:, pl.ds(n, WIDE)],
                    r["w"].at[:, pl.ds(n, WIDE)],
                    r["wsem"].at[i],
                ).wait()

        return

    if t < CHUNKS:

        @pl.when((chip == 0) & (core == 0))
        def _():
            for b in range(2):
                pltpu.make_async_copy(
                    r["hidden"].at[2 * t + b], r["sendR"].at[pl.ds(64 * b, 64)], r["xsem"].at[b]
                ).start()
            for b in range(2):
                pltpu.make_async_copy(
                    r["hidden"].at[2 * t + b], r["sendR"].at[pl.ds(64 * b, 64)], r["xsem"].at[b]
                ).wait()
            r["relay_ids"] = pair_ids(r["ids"], t)
            sums, counts = relay_layer(r, r["sendR"])
            add_stats(r["stats"], 0, sums, counts)

    if 2 <= t < CHUNKS + 2:

        @pl.when((chip == 0) & (core == 1))
        def _():
            r["cur"][...] = r["recvR"][...]
            r["relay_ids"] = pair_ids(r["ids"], t - 2)
            sums, counts = relay_layer(r, r["cur"])
            r["sendA"][...] = r["cur"][0:64, :]
            r["sendB"][...] = r["cur"][64:128, :]
            add_stats(r["stats"], 2, sums, counts)

    if t >= 4:
        chunk = t - 2 - 2 * chip
        active = (chip >= 1) & (chunk >= 0) & (chunk < CHUNKS)

        @pl.when(active)
        def _():
            cur = r["sendB"]
            if "recvA" in r:
                from_a = (chip == 1) & (core == 0)

                @pl.when(from_a)
                def _():
                    cur[...] = r["recvA"][...]

                @pl.when(jnp.logical_not(from_a))
                def _():
                    cur[...] = r["recvB"][...]
            else:
                cur[...] = r["recvB"][...]
            batch = 2 * chunk + core

            def one(layer, carry):
                own = layer == core
                small, other = r["small"], r["small_other"]

                def pick(rows, c, n):
                    return jnp.where(own, small[rows, c : c + n], other[rows, c : c + n])

                sums, counts = front(
                    64,
                    lambda c, n: cur[:, c : c + n],
                    lambda c, n: pick(slice(128, 129), c, n),
                    lambda: pick(slice(0, 60), 0, cur.shape[1]),
                    lambda c, n: pick(slice(64, 124), c, n),
                    jnp.where(own, r["ids"][batch], r["ids_other"][batch]),
                    r["nrm"],
                    r["nbf"],
                    r["mixed"],
                )
                for flag, w in ((own, r["w"]), (jnp.logical_not(own), r["w_other"])):

                    @pl.when(flag)
                    def _():
                        for n in range(0, cur.shape[1], WIDE):
                            mix_block(64, cur, r["mixed"], w, n)

                add_stats(r["stats"], 2 * layer, sums, counts)
                return carry

            lax.fori_loop(0, 2, one, 0)


IN_HBM = ("hidden", "w_hbm")


def run_step(t, ins, outs):
    names_in, names_out = tuple(ins), tuple(outs)
    rows = 128 if t < CHUNKS + 2 else 64
    scratch = {
        "nrm": pltpu.VMEM((rows, 2048), jnp.float32),
        "nbf": pltpu.VMEM((rows, 2048), jnp.bfloat16),
        "mixed": pltpu.VMEM((rows, 2048), jnp.bfloat16),
    }
    if 2 <= t < CHUNKS + 2:
        scratch["cur"] = pltpu.VMEM((128, 2048), jnp.bfloat16)
    if t < CHUNKS:
        scratch["xsem"] = pltpu.SemaphoreType.DMA((2,))
    if t == 0:
        scratch["wsem"] = pltpu.SemaphoreType.DMA((4,))
    space = {n: pltpu.HBM if n in IN_HBM else pltpu.VMEM for n in names_in}
    args = [pltpu.with_memory_space_constraint(ins[n], space[n]) for n in names_in]
    flops = 2 * 64 * 2048 * 2048 * 2
    got = pl.pallas_call(
        functools.partial(step_kernel, t, names_in, names_out, tuple(scratch)),
        out_shape=[pltpu.VMEM(*outs[n]) for n in names_out],
        in_specs=[pl.BlockSpec(memory_space=space[n]) for n in names_in],
        out_specs=[pl.BlockSpec(memory_space=pltpu.VMEM) for _ in names_out],
        scratch_shapes=list(scratch.values()),
        compiler_params=pltpu.CompilerParams(vmem_limit_bytes=VMEM_LIMIT),
        cost_estimate=pl.CostEstimate(
            flops=flops, bytes_accessed=8 * 1024 * 1024, transcendentals=0
        ),
        name=f"step{t}",
    )(*args)
    return dict(zip(names_out, got))


def hop_pairs(t):
    pairs = []
    if 2 <= t < CHUNKS + 2:
        pairs.append((1, 3))
    for chip in (1, 2, 3):
        chunk = t - 2 - 2 * chip
        if 0 <= chunk < CHUNKS:
            goal = chip + 1 if chip < CHIPS - 1 else chunk
            if goal != chip or chip < CHIPS - 1:
                pairs += [(2 * chip + c, 2 * goal + c) for c in range(2)]
    return pairs


def per_device(hidden_in, norm_gain, router_weight, expert_scale, mix_weight, routes):
    chip, core = lax.axis_index("x"), lax.axis_index("c")
    batches, rows, width = hidden_in.shape
    experts, picks = router_weight.shape[2], routes.shape[3]
    router = jnp.transpose(router_weight[0])
    ids = jnp.transpose(routes[0], (0, 2, 1))
    scale, w = expert_scale[0], mix_weight[0]
    swap = [(2 * x + c, 2 * x + 1 - c) for x in range(1, CHIPS) for c in range(2)]

    half = ((rows, width), jnp.bfloat16)
    full = ((2 * rows, width), jnp.bfloat16)
    stats_shape = ((experts, 128), jnp.float32)
    own = {"router": router, "scale": scale, "gain": norm_gain, "ids": ids}
    got = run_step(
        0,
        {"hidden": hidden_in, "w_hbm": w, **own},
        {
            "w": (w.shape, w.dtype),
            "sendR": full,
            "stats": stats_shape,
            "small": ((144, width), jnp.bfloat16),
        },
    )
    w_own, stats, small = got["w"], got["stats"], got["small"]
    recv = {("R", 0): lax.ppermute(got["sendR"], SEC, [(0, 1)])}
    w_other = lax.ppermute(w, SEC, swap)
    small_other = lax.ppermute(small, SEC, swap)
    ids_other = lax.ppermute(ids, SEC, swap)
    last = None
    for t in range(1, STEPS):
        ins, outs = {"stats_in": stats, "ids": ids, "w": w_own}, {"stats": stats_shape}
        if t < CHUNKS + 2:
            ins |= own
        if t < CHUNKS:
            ins["hidden"] = hidden_in
            outs["sendR"] = full
        if 2 <= t < CHUNKS + 2:
            ins["recvR"] = recv[("R", t - 2)]
            outs["sendA"] = half
        if t >= 2:
            outs["sendB"] = half
        if t >= 4:
            ins |= {"small": small, "small_other": small_other}
            ins |= {"w_other": w_other, "ids_other": ids_other}
            ins["recvB"] = recv[("B", t - 2)]
            if ("A", t - 2) in recv:
                ins["recvA"] = recv[("A", t - 2)]
        got = run_step(t, ins, outs)
        stats = got["stats"]
        if t < CHUNKS:
            recv[("R", t)] = lax.ppermute(got["sendR"], SEC, [(0, 1)])
        if 2 <= t < CHUNKS + 2:
            recv[("A", t)] = lax.ppermute(got["sendA"], SEC, [(1, 2)])
        if t >= 2 and t < STEPS - 1:
            recv[("B", t)] = lax.ppermute(got["sendB"], SEC, hop_pairs(t))
        if t == STEPS - 1:
            last = got["sendB"]
    out = last
    for k in range(CHUNKS - 1):
        out = jnp.where(chip == k, recv[("B", k + 8)], out)

    table = jnp.transpose(stats[:, 0:4]).reshape(2, 2 * experts)
    sent = jnp.repeat(table, lax.axis_size("z") * lax.axis_size("y"), axis=0)
    arrived = lax.all_to_all(sent, ("c", "z", "y"), 0, 0, tiled=True)
    total = jnp.sum(arrived, axis=0)
    prob_total, count_total = total[:experts], total[experts:]
    token_total = jnp.float32(batches * rows * lax.axis_size("z") * lax.axis_size("y"))
    fractions = count_total / (token_total * jnp.float32(picks))
    balance = jnp.float32(experts) * jnp.sum(fractions * (prob_total / token_total))
    return out[None], jnp.reshape(balance, (1,))


def solution(mesh):
    torus = Mesh(mesh.devices.reshape(CHIPS, 2, 8, 4), ("x", "c", "z", "y"))
    dp = ("z", "y")
    return jax.shard_map(
        per_device,
        mesh=torus,
        in_specs=(
            P(None, dp, None),
            P(SEC, None),
            P(SEC, None, None),
            P(SEC, None, None),
            P(SEC, None, None),
            P(SEC, None, dp, None),
        ),
        out_specs=(P(SEC, dp, None), P(SEC)),
        check_vma=False,
    )
```

```python
import functools

import jax
import jax.numpy as jnp
from jax import lax
from jax.experimental import pallas as pl
from jax.experimental.pallas import tpu as pltpu
from jax.sharding import Mesh
from jax.sharding import PartitionSpec as P


SEC = ("x", "c")
CHIPS = 4
CHUNKS = 4
STEPS = 12
COLS = 256
WIDE = 512
VMEM_LIMIT = 12 * 1024 * 1024


def front(rows, load_x, load_gain, load_router, load_scale, ids, nrm, nbf, mixed):
    width = nrm.shape[1]
    acc = None
    for c in range(0, width, COLS):
        xs = load_x(c, COLS).astype(jnp.float32)
        acc = xs * xs if acc is None else acc + xs * xs
    mean_square = jnp.sum(acc, axis=-1, keepdims=True) * jnp.float32(1.0 / width)
    inv = lax.rsqrt(mean_square + 1e-06)
    for c in range(0, width, COLS):
        xs = load_x(c, COLS).astype(jnp.float32)
        normed = xs * inv * load_gain(c, COLS).astype(jnp.float32)
        nrm[0:rows, c : c + COLS] = normed
        nbf[0:rows, c : c + COLS] = normed.astype(jnp.bfloat16)
    logits = lax.dot_general(
        load_router(),
        nbf[0:rows, :],
        (((1,), (1,)), ((), ())),
        preferred_element_type=jnp.float32,
    )
    exponent = jnp.exp(logits)
    probs = exponent / jnp.sum(exponent, axis=0, keepdims=True)
    expert = lax.broadcasted_iota(jnp.int32, probs.shape, 0)
    hit = ids[0:1, :] == expert
    for k in range(1, ids.shape[0]):
        hit = hit | (ids[k : k + 1, :] == expert)
    chosen = jnp.where(hit, 1.0, 0.0).astype(jnp.float32)
    gates = jnp.transpose(probs * chosen).astype(jnp.bfloat16)
    for c in range(0, width, COLS):
        channel = jnp.dot(gates, load_scale(c, COLS), preferred_element_type=jnp.float32)
        mixed[0:rows, c : c + COLS] = (nrm[0:rows, c : c + COLS] * channel).astype(jnp.bfloat16)
    return (
        jnp.sum(probs, axis=1, keepdims=True),
        jnp.sum(chosen, axis=1, keepdims=True),
    )


def mix_block(rows, cur, mixed, w, n, choice=None):
    weight = w[:, n : n + WIDE]
    if choice is not None:
        weight = jnp.where(choice[0], weight, choice[1][:, n : n + WIDE])
    update = jnp.dot(mixed[0:rows, :], weight, preferred_element_type=jnp.float32)
    cur[0:rows, n : n + WIDE] = (cur[0:rows, n : n + WIDE].astype(jnp.float32) + update).astype(
        jnp.bfloat16
    )


def add_stats(stats, lane, sums, counts):
    at = lax.broadcasted_iota(jnp.int32, stats.shape, 1)
    stats[...] += jnp.where(at == lane, sums, 0.0) + jnp.where(at == lane + 1, counts, 0.0)


def relay_layer(r, cur, ids, sems=None):
    rows = cur.shape[0]
    sums, counts = front(
        rows,
        lambda c, n: cur[0:rows, c : c + n],
        lambda c, n: r["gain"][:, c : c + n],
        lambda: r["router"][...],
        lambda c, n: r["scale"][:, c : c + n],
        ids,
        r["nrm"],
        r["nbf"],
        r["mixed"],
    )
    for i, n in enumerate(range(0, cur.shape[1], WIDE)):
        if sems is not None:
            weight_copy(r, sems, i, n).wait()
        mix_block(rows, cur, r["mixed"], r["w"], n)
    return sums, counts


SMALL = ("gain", "ids", "router", "scale")


def weight_copy(r, sems, i, n):
    return pltpu.make_async_copy(
        r["w_hbm"].at[:, pl.ds(n, WIDE)], r["w"].at[:, pl.ds(n, WIDE)], sems.at[i]
    )


def small_copies(r):
    return [
        pltpu.make_async_copy(r[n + "_hbm"], r[n], r["ssem"].at[i]) for i, n in enumerate(SMALL)
    ]


def load_own(r):
    for copy in small_copies(r):
        copy.start()
    for i, n in enumerate(range(0, r["w"].shape[1], WIDE)):
        weight_copy(r, r["wsem"], i, n).start()
    for copy in small_copies(r):
        copy.wait()


def wait_weight(r):
    for i, n in enumerate(range(0, r["w"].shape[1], WIDE)):
        weight_copy(r, r["wsem"], i, n).wait()


def hidden_copies(r, t, to):
    return [
        pltpu.make_async_copy(
            r["hidden"].at[2 * t + b], to.at[pl.ds(64 * b, 64)], r["xsem"].at[b]
        )
        for b in range(2)
    ]


def step_kernel(t, names_in, names_out, names_scratch, *refs):
    ins = dict(zip(names_in, refs))
    outs = dict(zip(names_out, refs[len(names_in) :]))
    r = ins | outs | dict(zip(names_scratch, refs[len(names_in) + len(names_out) :]))
    chip, core = lax.axis_index("x"), lax.axis_index("c")
    if "stats_in" in r:
        r["stats"][...] = r["stats_in"][...]
    else:
        r["stats"][...] = jnp.zeros_like(r["stats"])

    def pair_ids(chunk):
        return jnp.concatenate([r["ids"][2 * chunk], r["ids"][2 * chunk + 1]], axis=1)

    if t == 0:

        @pl.when((chip == 0) & (core == 0))
        def _():
            for copy in hidden_copies(r, 0, r["sendR"]):
                copy.start()
            load_own(r)
            for copy in hidden_copies(r, 0, r["sendR"]):
                copy.wait()
            sums, counts = relay_layer(r, r["sendR"], pair_ids(0), r["wsem"])
            add_stats(r["stats"], 0, sums, counts)

        @pl.when((chip == 0) & (core == 1))
        def _():
            load_own(r)
            wait_weight(r)

    if t == 1:

        @pl.when(chip > 0)
        def _():
            load_own(r)
            r["small"][0:60, :] = r["router"][...]
            r["small"][64:124, :] = r["scale"][...]
            r["small"][128:129, :] = r["gain"][...]
            wait_weight(r)

    if 1 <= t < CHUNKS + 2:
        cur = r["cur"] if "cur" in r else r["sendR"]
        first, second = (chip == 0) & (core == 0), (chip == 0) & (core == 1)
        chunk = t - 2 * core
        if t < CHUNKS:

            @pl.when(first)
            def _():
                for copy in hidden_copies(r, t, cur):
                    copy.start()
                for copy in hidden_copies(r, t, cur):
                    copy.wait()

        if t >= 2:

            @pl.when(second)
            def _():
                cur[...] = r["recvR"][...]

        @pl.when(first if t < 2 else (second if t >= CHUNKS else chip == 0))
        def _():
            sums, counts = relay_layer(r, cur, pair_ids(chunk))
            add_stats(r["stats"], 2 * core, sums, counts)

        if 2 <= t < CHUNKS:

            @pl.when(first)
            def _():
                r["sendR"][...] = cur[...]

        if t >= 2:

            @pl.when(second)
            def _():
                r["sendA"][...] = cur[0:64, :]
                r["sendB"][...] = cur[64:128, :]

    if t >= 4:
        chunk = t - 2 - 2 * chip
        active = (chip >= 1) & (chunk >= 0) & (chunk < CHUNKS)

        @pl.when(active)
        def _():
            cur = r["sendB"]
            if "recvA" in r:
                from_a = (chip == 1) & (core == 0)

                @pl.when(from_a)
                def _():
                    cur[...] = r["recvA"][...]

                @pl.when(jnp.logical_not(from_a))
                def _():
                    cur[...] = r["recvB"][...]
            else:
                cur[...] = r["recvB"][...]
            batch = 2 * chunk + core

            def one(layer, carry):
                own = layer == core
                small, other = r["small"], r["small_other"]

                def pick(rows, c, n):
                    return jnp.where(own, small[rows, c : c + n], other[rows, c : c + n])

                sums, counts = front(
                    64,
                    lambda c, n: cur[:, c : c + n],
                    lambda c, n: pick(slice(128, 129), c, n),
                    lambda: pick(slice(0, 60), 0, cur.shape[1]),
                    lambda c, n: pick(slice(64, 124), c, n),
                    jnp.where(own, r["ids"][batch], r["ids_other"][batch]),
                    r["nrm"],
                    r["nbf"],
                    r["mixed"],
                )
                for n in range(0, cur.shape[1], WIDE):
                    mix_block(64, cur, r["mixed"], r["w"], n, (own, r["w_other"]))

                add_stats(r["stats"], 2 * layer, sums, counts)
                return carry

            lax.fori_loop(0, 2, one, 0)


    if t == STEPS - 1:
        table = jnp.transpose(
            jnp.concatenate([r["stats"][...], jnp.zeros((128 - 60, 128), jnp.float32)], axis=0)
        )
        for layer in range(2):
            row = table[2 * layer : 2 * layer + 1, :]
            counts = table[2 * layer + 1 : 2 * layer + 2, :]
            at = lax.broadcasted_iota(jnp.int32, row.shape, 1)
            row = jnp.where(at < 60, row, jnp.where(at >= 64, pltpu.roll(counts, 64, 1), 0.0))
            r["table"][32 * layer : 32 * layer + 32, :] = jnp.broadcast_to(row, (32, 128))


def final_kernel(token_total, *refs):
    arrived, parts, last, out, balance, sem = refs[0], refs[1:4], refs[4], *refs[5:8]
    chip = lax.axis_index("x")
    for k, part in enumerate((*parts, last)):

        @pl.when(chip == k)
        def _():
            pltpu.make_async_copy(part, out, sem).start()

    total = jnp.sum(arrived[...], axis=0, keepdims=True)
    counts = pltpu.roll(total, 64, 1)
    at = lax.broadcasted_iota(jnp.int32, total.shape, 1)
    terms = jnp.where(at < 60, (counts / (token_total * 4.0)) * (total / token_total), 0.0)
    balance[0] = 60.0 * jnp.sum(terms)
    pltpu.make_async_copy(last, out, sem).wait()


def call(kernel, ins, outs, scratch, flops, aliases=()):
    names_in, names_out = tuple(ins), tuple(outs)
    space = {n: pltpu.HBM if n.endswith("_hbm") or n == "hidden" else pltpu.VMEM for n in ins}
    args = [pltpu.with_memory_space_constraint(ins[n], space[n]) for n in names_in]
    place = {"out": pltpu.HBM, "balance": pltpu.SMEM}
    out_space = {n: place.get(n, pltpu.VMEM) for n in outs}
    got = pl.pallas_call(
        kernel,
        out_shape=[out_space[n](*outs[n]) for n in names_out],
        in_specs=[pl.BlockSpec(memory_space=space[n]) for n in names_in],
        out_specs=[pl.BlockSpec(memory_space=out_space[n]) for n in names_out],
        scratch_shapes=list(scratch.values()),
        input_output_aliases={names_in.index(a): names_out.index(b) for a, b in aliases},
        compiler_params=pltpu.CompilerParams(vmem_limit_bytes=VMEM_LIMIT),
        cost_estimate=pl.CostEstimate(
            flops=flops, bytes_accessed=8 * 1024 * 1024, transcendentals=0
        ),
    )(*args)
    return dict(zip(names_out, got))


def run_step(t, ins, outs, aliases=()):
    rows = 128 if t < CHUNKS + 2 else 64
    scratch = {
        "nrm": pltpu.VMEM((rows, 2048), jnp.float32),
        "nbf": pltpu.VMEM((rows, 2048), jnp.bfloat16),
        "mixed": pltpu.VMEM((rows, 2048), jnp.bfloat16),
    }
    if 2 <= t < CHUNKS + 2:
        scratch["cur"] = pltpu.VMEM((128, 2048), jnp.bfloat16)
    if t < CHUNKS:
        scratch["xsem"] = pltpu.SemaphoreType.DMA((2,))
    if "stats" not in outs:
        scratch["stats"] = pltpu.VMEM((60, 128), jnp.float32)
    if t < 2:
        scratch["wsem"] = pltpu.SemaphoreType.DMA((4,))
        scratch["ssem"] = pltpu.SemaphoreType.DMA((4,))
    kernel = functools.partial(step_kernel, t, tuple(ins), tuple(outs), tuple(scratch))
    return call(kernel, ins, outs, scratch, 2 * 64 * 2048 * 2048 * 2, aliases)


def hop_pairs(t):
    pairs = []
    if 2 <= t < CHUNKS + 2:
        pairs.append((1, 3))
    for chip in (1, 2, 3):
        chunk = t - 2 - 2 * chip
        if 0 <= chunk < CHUNKS:
            goal = chip + 1 if chip < CHIPS - 1 else chunk
            if goal != chip or chip < CHIPS - 1:
                pairs += [(2 * chip + c, 2 * goal + c) for c in range(2)]
    return pairs


def per_device(hidden_in, norm_gain, router_weight, expert_scale, mix_weight, routes):
    batches, rows, width = hidden_in.shape
    experts = router_weight.shape[2]
    router = jnp.transpose(router_weight[0])
    ids = jnp.transpose(routes[0], (0, 2, 1))
    scale, w = expert_scale[0], mix_weight[0]
    swap = [(2 * x + c, 2 * x + 1 - c) for x in range(1, CHIPS) for c in range(2)]

    def hop(x, pairs):
        return lax.ppermute(x, SEC, pairs)

    half = ((rows, width), jnp.bfloat16)
    full = ((2 * rows, width), jnp.bfloat16)
    stats_shape = ((experts, 128), jnp.float32)
    own = {"w": w, "router": router, "scale": scale, "gain": norm_gain, "ids": ids}
    own_hbm = {n + "_hbm": v for n, v in own.items()}
    own_shapes = {n: (v.shape, v.dtype) for n, v in own.items()}
    got = run_step(
        0,
        {"hidden": hidden_in, **own_hbm},
        {**own_shapes, "sendR": full, "stats": stats_shape},
    )
    recv = {("R", 0): hop(got["sendR"], [(0, 1)])}
    w_other = hop(w, swap)
    ids_other = hop(ids, swap)
    got = run_step(
        1,
        {
            "stats_in": got["stats"],
            "hidden": hidden_in,
            **own_hbm,
            **{n + "_in": got[n] for n in own},
        },
        {**own_shapes, "sendR": full, "stats": stats_shape, "small": ((144, width), jnp.bfloat16)},
        [(n + "_in", n) for n in own],
    )
    recv[("R", 1)] = hop(got["sendR"], [(0, 1)])
    small, stats, own = got["small"], got["stats"], {n: got[n] for n in own}
    small_other = hop(small, swap)
    last = None
    for t in range(2, STEPS):
        ins = {"stats_in": stats, "ids": own["ids"], "w": own["w"]}
        outs = {"stats": stats_shape, "sendB": half}
        if t < CHUNKS + 2:
            ins |= own
            ins["recvR"] = recv[("R", t - 2)]
            outs["sendA"] = half
        if t < CHUNKS:
            ins["hidden"] = hidden_in
            outs["sendR"] = full
        if t >= 4:
            ins |= {"small": small, "small_other": small_other}
            ins |= {"w_other": w_other, "ids_other": ids_other}
            ins["recvB"] = recv[("B", t - 2)]
            if ("A", t - 2) in recv:
                ins["recvA"] = recv[("A", t - 2)]
        if t == STEPS - 1:
            outs = {"sendB": half, "table": ((2 * 32, 128), jnp.float32)}
        got = run_step(t, ins, outs)
        stats, last = got.get("stats"), got["sendB"]
        if t < STEPS - 1:
            recv[("B", t)] = hop(got["sendB"], hop_pairs(t))
        if 2 <= t < CHUNKS + 2:
            recv[("A", t)] = hop(got["sendA"], [(1, 2)])
        if t < CHUNKS:
            recv[("R", t)] = hop(got["sendR"], [(0, 1)])
    arrived = lax.all_to_all(got["table"], ("c", "z", "y"), 0, 0, tiled=True)
    token_total = float(batches * rows * lax.axis_size("z") * lax.axis_size("y"))
    got = call(
        functools.partial(final_kernel, token_total),
        {
            "arrived": arrived,
            **{f"part{k}": recv[("B", k + 8)] for k in range(CHUNKS - 1)},
            "last": last,
        },
        {"out": half, "balance": ((1,), jnp.float32)},
        {"sem": pltpu.SemaphoreType.DMA},
        1000,
    )
    return got["out"][None], got["balance"]


def solution(mesh):
    torus = Mesh(mesh.devices.reshape(CHIPS, 2, 8, 4), ("x", "c", "z", "y"))
    dp = ("z", "y")

    return jax.shard_map(
        per_device,
        mesh=torus,
        in_specs=(
            P(None, dp, None),
            P(SEC, None),
            P(SEC, None, None),
            P(SEC, None, None),
            P(SEC, None, None),
            P(SEC, None, dp, None),
        ),
        out_specs=(P(SEC, dp, None), P(SEC)),
        check_vma=False,
    )
```

```python
import functools

import jax
import jax.numpy as jnp
from jax import lax
from jax.experimental import pallas as pl
from jax.experimental.pallas import tpu as pltpu
from jax.sharding import Mesh
from jax.sharding import PartitionSpec as P


SEC = ("x", "c")
CHIPS = 4
CHUNKS = 4
STEPS = 13
LAST_RELAY = 7
FIRST_PAIR = 5
COLS = 256
WIDE = 512
VMEM_LIMIT = 12 * 1024 * 1024


def front(rows, load_x, load_gain, load_router, load_scale, ids, nrm, nbf, mixed):
    width = nrm.shape[1]
    acc = None
    for c in range(0, width, COLS):
        xs = load_x(c, COLS).astype(jnp.float32)
        acc = xs * xs if acc is None else acc + xs * xs
    mean_square = jnp.sum(acc, axis=-1, keepdims=True) * jnp.float32(1.0 / width)
    inv = lax.rsqrt(mean_square + 1e-06)
    for c in range(0, width, COLS):
        xs = load_x(c, COLS).astype(jnp.float32)
        normed = xs * inv * load_gain(c, COLS).astype(jnp.float32)
        nrm[0:rows, c : c + COLS] = normed
        nbf[0:rows, c : c + COLS] = normed.astype(jnp.bfloat16)
    logits = lax.dot_general(
        load_router(),
        nbf[0:rows, :],
        (((1,), (1,)), ((), ())),
        preferred_element_type=jnp.float32,
    )
    exponent = jnp.exp(logits)
    probs = exponent / jnp.sum(exponent, axis=0, keepdims=True)
    expert = lax.broadcasted_iota(jnp.int32, probs.shape, 0)
    hit = ids[0:1, :] == expert
    for k in range(1, ids.shape[0]):
        hit = hit | (ids[k : k + 1, :] == expert)
    chosen = jnp.where(hit, 1.0, 0.0).astype(jnp.float32)
    gates = jnp.transpose(probs * chosen).astype(jnp.bfloat16)
    for c in range(0, width, COLS):
        channel = jnp.dot(gates, load_scale(c, COLS), preferred_element_type=jnp.float32)
        mixed[0:rows, c : c + COLS] = (nrm[0:rows, c : c + COLS] * channel).astype(jnp.bfloat16)
    return (
        jnp.sum(probs, axis=1, keepdims=True),
        jnp.sum(chosen, axis=1, keepdims=True),
    )


def mix_block(rows, cur, mixed, w, n, choice=None):
    weight = w[:, n : n + WIDE]
    if choice is not None:
        weight = jnp.where(choice[0], weight, choice[1][:, n : n + WIDE])
    update = jnp.dot(mixed[0:rows, :], weight, preferred_element_type=jnp.float32)
    cur[0:rows, n : n + WIDE] = (cur[0:rows, n : n + WIDE].astype(jnp.float32) + update).astype(
        jnp.bfloat16
    )


def add_stats(stats, lane, sums, counts):
    at = lax.broadcasted_iota(jnp.int32, stats.shape, 1)
    stats[...] += jnp.where(at == lane, sums, 0.0) + jnp.where(at == lane + 1, counts, 0.0)


def relay_layer(r, cur, ids, sems=None):
    rows = cur.shape[0]
    sums, counts = front(
        rows,
        lambda c, n: cur[0:rows, c : c + n],
        lambda c, n: r["gain"][:, c : c + n],
        lambda: r["router"][...],
        lambda c, n: r["scale"][:, c : c + n],
        ids,
        r["nrm"],
        r["nbf"],
        r["mixed"],
    )
    if rows > 64:

        def block(i, carry):
            at = pl.ds(pl.multiple_of(i * WIDE, WIDE), WIDE)
            update = jnp.dot(
                r["mixed"][0:rows, :], r["w"][:, at], preferred_element_type=jnp.float32
            )
            cur[0:rows, at] = (cur[0:rows, at].astype(jnp.float32) + update).astype(jnp.bfloat16)
            return carry

        lax.fori_loop(0, cur.shape[1] // WIDE, block, 0)
        return sums, counts
    for i, n in enumerate(range(0, cur.shape[1], WIDE)):
        if sems is not None:
            weight_copy(r, sems, i, n).wait()
        mix_block(rows, cur, r["mixed"], r["w"], n)
    return sums, counts


SMALL = ("gain", "ids", "router", "scale")


def weight_copy(r, sems, i, n):
    return pltpu.make_async_copy(
        r["w_hbm"].at[:, pl.ds(n, WIDE)], r["w"].at[:, pl.ds(n, WIDE)], sems.at[i]
    )


def weight_copies(r):
    width = r["w"].shape[1]
    return [weight_copy(r, r["wsem"], i, n) for i, n in enumerate(range(0, width, WIDE))]


def small_copies(r):
    return [
        pltpu.make_async_copy(r[n + "_hbm"], r[n], r["ssem"].at[i]) for i, n in enumerate(SMALL)
    ]


def hidden_copies(r, first, to):
    return [
        pltpu.make_async_copy(
            r["hidden"].at[first + b], to.at[pl.ds(64 * b, 64)], r["xsem"].at[b]
        )
        for b in range(to.shape[0] // 64)
    ]


def load_hidden(r, first, to):
    for copy in hidden_copies(r, first, to):
        copy.start()
    for copy in hidden_copies(r, first, to):
        copy.wait()


def pair_ids(r, chunk):
    return jnp.concatenate([r["ids"][2 * chunk], r["ids"][2 * chunk + 1]], axis=1)


def first_step(r, first, second):
    for copy in small_copies(r):
        copy.start()

    @pl.when(first)
    def _():
        load_hidden(r, 0, r["sendR"])

    for copy in small_copies(r):
        copy.wait()

    @pl.when(first | second)
    def _():
        for copy in weight_copies(r):
            copy.start()

    @pl.when(first)
    def _():
        sums, counts = relay_layer(r, r["sendR"], r["ids"][0], r["wsem"])
        add_stats(r["stats"], 0, sums, counts)

    @pl.when(second)
    def _():
        for copy in weight_copies(r):
            copy.wait()

    @pl.when(jnp.logical_not(first | second))
    def _():
        ids = jnp.concatenate([r["ids"][m] for m in range(r["ids"].shape[0])], axis=0)
        r["small"][0:60, :] = r["router"][...]
        r["small"][64:124, :] = r["scale"][...]
        r["small"][128:129, :] = r["gain"][...]
        r["small"][144:176, 0:64] = ids.astype(jnp.float32).astype(jnp.bfloat16)


def relay_step(t, r, first, second, core):
    if t == 1:

        @pl.when(first)
        def _():
            load_hidden(r, 1, r["sendR"])
            sums, counts = relay_layer(r, r["sendR"], r["ids"][1])
            add_stats(r["stats"], 0, sums, counts)

    if t in (2, 3):

        @pl.when(first)
        def _():
            load_hidden(r, 2 * (t - 1), r["sendR"])
            sums, counts = relay_layer(r, r["sendR"], pair_ids(r, t - 1))
            add_stats(r["stats"], 0, sums, counts)

        @pl.when(second)
        def _():
            cur = r["sendA"] if t == 2 else r["sendB"]
            cur[...] = r["recvR"][...]
            sums, counts = relay_layer(r, cur, r["ids"][t - 2])
            add_stats(r["stats"], 2, sums, counts)

    if 4 <= t < LAST_RELAY:
        cur = r["cur"]
        if t == 4:

            @pl.when(first)
            def _():
                load_hidden(r, 2 * (t - 1), cur)

        @pl.when(second)
        def _():
            cur[...] = r["recvR"][...]

        @pl.when((first | second) if t == 4 else second)
        def _():
            sums, counts = relay_layer(r, cur, pair_ids(r, t - 1 - 2 * core))
            add_stats(r["stats"], 2 * core, sums, counts)

        if t == 4:

            @pl.when(first)
            def _():
                r["sendR"][...] = cur[...]

        @pl.when(second)
        def _():
            r["sendA"][...] = cur[0:64, :]
            r["sendB"][...] = cur[64:128, :]


def pair_step(t, r, chip, core):
    chunk = t - 3 - 2 * chip
    cur = r["sendB"]

    @pl.when((chip >= 1) & (chunk >= 0) & (chunk < CHUNKS))
    def _():
        if "recvA" in r:
            from_a = (chip == 1) & (core == 0)

            @pl.when(from_a)
            def _():
                cur[...] = r["recvA"][...]

            @pl.when(jnp.logical_not(from_a))
            def _():
                cur[...] = r["recvB"][...]
        else:
            cur[...] = r["recvB"][...]
        batch = 2 * chunk + core
        small, other = r["small"], r["small_other"]

        def one(layer, carry):
            own = layer == core

            def pick(rows, c, n):
                return jnp.where(own, small[rows, c : c + n], other[rows, c : c + n])

            table = pick(slice(144, 176), 0, 64).astype(jnp.float32)
            ids = table[0:4]
            for m in range(1, 8):
                ids = jnp.where(batch == m, table[4 * m : 4 * m + 4], ids)
            sums, counts = front(
                64,
                lambda c, n: cur[:, c : c + n],
                lambda c, n: pick(slice(128, 129), c, n),
                lambda: pick(slice(0, 60), 0, cur.shape[1]),
                lambda c, n: pick(slice(64, 124), c, n),
                ids.astype(jnp.int32),
                r["nrm"],
                r["nbf"],
                r["mixed"],
            )

            def mix():
                for n in range(0, cur.shape[1], WIDE):
                    mix_block(64, cur, r["mixed"], r["w"], n, (own, r["w_other"]))

            if t == STEPS - 1:
                pl.when(layer == 0)(mix)
            else:
                mix()
            add_stats(r["stats"], 2 * layer, sums, counts)
            return carry

        lax.fori_loop(0, 2, one, 0)


def stats_table(r):
    table = jnp.transpose(
        jnp.concatenate([r["stats"][...], jnp.zeros((128 - 60, 128), jnp.float32)], axis=0)
    )
    for layer in range(2):
        row = table[2 * layer : 2 * layer + 1, :]
        counts = table[2 * layer + 1 : 2 * layer + 2, :]
        at = lax.broadcasted_iota(jnp.int32, row.shape, 1)
        row = jnp.where(at < 60, row, jnp.where(at >= 64, pltpu.roll(counts, 64, 1), 0.0))
        r["table"][32 * layer : 32 * layer + 32, :] = jnp.broadcast_to(row, (32, 128))


def step_kernel(t, names, *refs):
    r = dict(zip(names, refs))
    chip, core = lax.axis_index("x"), lax.axis_index("c")
    first, second = (chip == 0) & (core == 0), (chip == 0) & (core == 1)
    if "stats_in" in r:
        r["stats"][...] = r["stats_in"][...]
    else:
        r["stats"][...] = jnp.zeros_like(r["stats"])
    if t == 0:
        first_step(r, first, second)
    elif t < LAST_RELAY:
        relay_step(t, r | {"w": r["w_relay"]}, first, second, core)
    if t >= FIRST_PAIR:
        pair_step(t, r, chip, core)
    if t == STEPS - 1:
        stats_table(r)


def tail_kernel(names, *refs):
    r = dict(zip(names, refs))
    chip, core = lax.axis_index("x"), lax.axis_index("c")
    for k in range(CHIPS - 1):

        @pl.when(chip == k)
        def _():
            pltpu.make_async_copy(r[f"part{k}"], r["out"], r["sem"]).start()

    blocks = list(enumerate(range(0, r["cur"].shape[1], WIDE)))
    for own, source in ((True, r["w_hbm"]), (False, r["w_other_hbm"])):

        @pl.when((chip == CHIPS - 1) & ((core == 1) if own else (core == 0)))
        def _():
            for i, n in blocks:
                weight_copy({"w_hbm": source, "w": r["w"]}, r["wsem"], i, n).start()

    @pl.when(chip == CHIPS - 1)
    def _():
        r["cur"][...] = r["mid"][...]
        for i, n in blocks:
            weight_copy({"w_hbm": r["w_hbm"], "w": r["w"]}, r["wsem"], i, n).wait()
            mix_block(64, r["cur"], r["mixed"], r["w"], n)
        pltpu.make_async_copy(r["cur"], r["out"], r["sem"]).start()

    pltpu.make_async_copy(r["cur"], r["out"], r["sem"]).wait()


def loss_kernel(token_total, arrived, balance):
    total = jnp.sum(arrived[...], axis=0, keepdims=True)
    counts = pltpu.roll(total, 64, 1)
    at = lax.broadcasted_iota(jnp.int32, total.shape, 1)
    terms = jnp.where(at < 60, (counts / (token_total * 4.0)) * (total / token_total), 0.0)
    balance[0] = 60.0 * jnp.sum(terms)


def call(kernel, ins, outs, scratch, flops):
    names_in, names_out = tuple(ins), tuple(outs)
    space = {n: pltpu.HBM if n.endswith("_hbm") or n == "hidden" else pltpu.VMEM for n in ins}
    args = [pltpu.with_memory_space_constraint(ins[n], space[n]) for n in names_in]
    place = {"out": pltpu.HBM, "balance": pltpu.SMEM}
    out_space = {n: place.get(n, pltpu.VMEM) for n in outs}
    got = pl.pallas_call(
        kernel,
        out_shape=[out_space[n](*outs[n]) for n in names_out],
        in_specs=[pl.BlockSpec(memory_space=space[n]) for n in names_in],
        out_specs=[pl.BlockSpec(memory_space=out_space[n]) for n in names_out],
        scratch_shapes=list(scratch.values()),
        compiler_params=pltpu.CompilerParams(vmem_limit_bytes=VMEM_LIMIT),
        cost_estimate=pl.CostEstimate(
            flops=flops, bytes_accessed=8 * 1024 * 1024, transcendentals=0
        ),
    )(*args)
    return dict(zip(names_out, got))


def run_step(t, ins, outs):
    rows = 128 if 2 <= t < LAST_RELAY else 64
    scratch = {
        "nrm": pltpu.VMEM((rows, 2048), jnp.float32),
        "nbf": pltpu.VMEM((rows, 2048), jnp.bfloat16),
    }
    if "mixed" not in outs:
        scratch["mixed"] = pltpu.VMEM((rows, 2048), jnp.bfloat16)
    if 4 <= t < LAST_RELAY:
        scratch["cur"] = pltpu.VMEM((128, 2048), jnp.bfloat16)
    if t < 5:
        scratch["xsem"] = pltpu.SemaphoreType.DMA((2,))
    if "stats" not in outs:
        scratch["stats"] = pltpu.VMEM((60, 128), jnp.float32)
    if t == 0:
        scratch["wsem"] = pltpu.SemaphoreType.DMA((4,))
        scratch["ssem"] = pltpu.SemaphoreType.DMA((4,))
    kernel = functools.partial(step_kernel, t, (*ins, *outs, *scratch))
    return call(kernel, ins, outs, scratch, 2 * 64 * 2048 * 2048 * 2)


def hop_pairs(t):
    pairs = [(1, 3)] if 3 <= t < LAST_RELAY else []
    for chip in (1, 2, 3):
        chunk = t - 3 - 2 * chip
        if 0 <= chunk < CHUNKS:
            goal = chip + 1 if chip < CHIPS - 1 else chunk
            pairs += [(2 * chip + c, 2 * goal + c) for c in range(2)]
    return pairs


def per_device(hidden_in, norm_gain, router_weight, expert_scale, mix_weight, routes):
    batches, rows, width = hidden_in.shape
    experts = router_weight.shape[2]
    router = jnp.transpose(router_weight[0])
    ids = jnp.transpose(routes[0], (0, 2, 1))
    scale, w = expert_scale[0], mix_weight[0]
    swap = [(2 * x + c, 2 * x + 1 - c) for x in range(1, CHIPS) for c in range(2)]

    def hop(x, pairs):
        return lax.ppermute(x, SEC, pairs)

    half = ((rows, width), jnp.bfloat16)
    full = ((2 * rows, width), jnp.bfloat16)
    stats_shape = ((experts, 128), jnp.float32)
    own = {"w": w, "router": router, "scale": scale, "gain": norm_gain, "ids": ids}
    w_other = hop(w, swap)
    got = run_step(
        0,
        {"hidden": hidden_in, **{n + "_hbm": v for n, v in own.items()}},
        {
            **{n: (v.shape, v.dtype) for n, v in own.items()},
            "sendR": half,
            "stats": stats_shape,
            "small": ((176, width), jnp.bfloat16),
        },
    )
    small, stats = got["small"], got["stats"]
    relay = {("w_relay" if n == "w" else n): got[n] for n in own}
    recv = {("R", 0): hop(got["sendR"], [(0, 1)])}
    for t in range(1, STEPS):
        ins, outs = {"stats_in": stats}, {"stats": stats_shape}
        if t < LAST_RELAY:
            ins |= relay
        if t < 5:
            ins["hidden"] = hidden_in
            outs["sendR"] = half if t == 1 else full
        if 2 <= t < LAST_RELAY:
            ins["recvR"] = recv[("R", t - 2)]
        if t in (2, 4, 5, 6):
            outs["sendA"] = half
        if t >= 3:
            outs["sendB"] = half
        if t >= FIRST_PAIR:
            ins |= {"small": small, "small_other": small_other, "w": w, "w_other": w_other}
            ins["recvB"] = recv[("B", t - 2)]
            at = 2 if t == FIRST_PAIR else t - 2
            if ("A", at) in recv:
                ins["recvA"] = recv[("A", at)]
        if t == STEPS - 1:
            outs = {"sendB": half, "mixed": half, "table": ((2 * 32, 128), jnp.float32)}
        got = run_step(t, ins, outs)
        stats = got.get("stats")
        if "sendA" in got:
            recv[("A", t)] = hop(got["sendA"], [(1, 2)])
        if t < STEPS - 1 and "sendB" in got:
            recv[("B", t)] = hop(got["sendB"], hop_pairs(t))
        if "sendR" in got:
            recv[("R", t)] = hop(got["sendR"], [(0, 1)])
        if t == 2:
            small_other = hop(small, swap)
    arrived = lax.all_to_all(got["table"], ("c", "z", "y"), 0, 0, tiled=True)
    ins = {f"part{k}": recv[("B", k + 9)] for k in range(CHUNKS - 1)}
    ins |= {"mid": got["sendB"], "mixed": got["mixed"], "w_hbm": w, "w_other_hbm": w_other}
    scratch = {"cur": pltpu.VMEM(*half), "w": pltpu.VMEM(w.shape, w.dtype)}
    scratch |= {"sem": pltpu.SemaphoreType.DMA, "wsem": pltpu.SemaphoreType.DMA((4,))}
    kernel = functools.partial(tail_kernel, (*ins, "out", *scratch))
    out = call(kernel, ins, {"out": half}, scratch, 2 * 64 * 2048 * 2048)["out"]
    token_total = float(batches * rows * lax.axis_size("z") * lax.axis_size("y"))
    kernel = functools.partial(loss_kernel, token_total)
    loss = call(kernel, {"arrived": arrived}, {"balance": ((1,), jnp.float32)}, {}, 1000)
    return out[None], loss["balance"]


def solution(mesh):
    torus = Mesh(mesh.devices.reshape(CHIPS, 2, 8, 4), ("x", "c", "z", "y"))
    dp = ("z", "y")

    return jax.shard_map(
        per_device,
        mesh=torus,
        in_specs=(
            P(None, dp, None),
            P(SEC, None),
            P(SEC, None, None),
            P(SEC, None, None),
            P(SEC, None, None),
            P(SEC, None, dp, None),
        ),
        out_specs=(P(SEC, dp, None), P(SEC)),
        check_vma=False,
    )
```

```python
import functools
from types import SimpleNamespace

import jax
import jax.numpy as jnp
from jax import lax
from jax.experimental import pallas as pl
from jax.experimental.pallas import tpu as pltpu
from jax.sharding import Mesh
from jax.sharding import PartitionSpec as P


X, C, Z, Y = "xczy"
SEC = (X, C)
CHIPS = 4
CHUNKS = 4
RELAY_END = 6
PAIR_START = 4
STEPS = 12
COLS = 256
WIDE = 512
VMEM_LIMIT = 12 * 1024 * 1024


def front(rows, load_x, load_gain, load_router, load_scale, ids, r):
    width = r.nrm.shape[1]
    acc = None
    for c in range(0, width, COLS):
        xs = load_x(c, COLS).astype(jnp.float32)
        acc = xs * xs if acc is None else acc + xs * xs
    mean_square = jnp.sum(acc, axis=-1, keepdims=True) * jnp.float32(1.0 / width)
    inv = lax.rsqrt(mean_square + 1e-06)
    for c in range(0, width, COLS):
        xs = load_x(c, COLS).astype(jnp.float32)
        normed = xs * inv * load_gain(c, COLS).astype(jnp.float32)
        r.nrm[0:rows, c : c + COLS] = normed
        r.nbf[0:rows, c : c + COLS] = normed.astype(jnp.bfloat16)
    logits = lax.dot_general(
        load_router(),
        r.nbf[0:rows, :],
        (((1,), (1,)), ((), ())),
        preferred_element_type=jnp.float32,
    )
    exponent = jnp.exp(logits)
    probs = exponent / jnp.sum(exponent, axis=0, keepdims=True)
    expert = lax.broadcasted_iota(jnp.int32, probs.shape, 0)
    hit = ids[0:1, :] == expert
    for k in range(1, ids.shape[0]):
        hit = hit | (ids[k : k + 1, :] == expert)
    chosen = jnp.where(hit, 1.0, 0.0).astype(jnp.float32)
    gates = jnp.transpose(probs * chosen).astype(jnp.bfloat16)
    for c in range(0, width, COLS):
        channel = jnp.dot(gates, load_scale(c, COLS), preferred_element_type=jnp.float32)
        r.mixed[0:rows, c : c + COLS] = (r.nrm[0:rows, c : c + COLS] * channel).astype(
            jnp.bfloat16
        )
    return (
        jnp.sum(probs, axis=1, keepdims=True),
        jnp.sum(chosen, axis=1, keepdims=True),
    )


def mix_block(rows, cur, mixed, w, n, choice=None):
    weight = w[:, n : n + WIDE]
    if choice is not None:
        weight = jnp.where(choice[0], weight, choice[1][:, n : n + WIDE])
    update = jnp.dot(mixed[0:rows, :], weight, preferred_element_type=jnp.float32)
    cur[0:rows, n : n + WIDE] = (cur[0:rows, n : n + WIDE].astype(jnp.float32) + update).astype(
        jnp.bfloat16
    )


def add_stats(stats, lane, sums, counts):
    at = lax.broadcasted_iota(jnp.int32, stats.shape, 1)
    stats[...] += jnp.where(at == lane, sums, 0.0) + jnp.where(at == lane + 1, counts, 0.0)


def relay_layer(r, cur, chunk, weight, waits=None):
    rows = cur.shape[0]
    sums, counts = front(
        rows,
        lambda c, n: cur[0:rows, c : c + n],
        lambda c, n: r.gain[:, c : c + n],
        lambda: r.router[...],
        lambda c, n: r.scale[:, c : c + n],
        jnp.concatenate([r.ids[2 * chunk], r.ids[2 * chunk + 1]], axis=1),
        r,
    )
    for i, n in enumerate(range(0, cur.shape[1], WIDE)):
        if waits is not None:
            waits[i].wait()
        mix_block(rows, cur, r.mixed, weight, n)
    return sums, counts


def column_copies(source, to, sems):
    return [
        pltpu.make_async_copy(source.at[:, pl.ds(n, WIDE)], to.at[:, pl.ds(n, WIDE)], sems.at[i])
        for i, n in enumerate(range(0, to.shape[1], WIDE))
    ]


def run_all(copies):
    for copy in copies:
        copy.start()
    for copy in copies:
        copy.wait()


def hidden_copies(r, chunk, to):
    return [
        pltpu.make_async_copy(r.hidden.at[2 * chunk + b], to.at[pl.ds(64 * b, 64)], r.xsem.at[b])
        for b in range(2)
    ]


def first_step(r, first, second):
    pairs = ((r.gain0, r.gain), (r.ids0, r.ids), (r.router0, r.router), (r.scale0, r.scale))
    small = [pltpu.make_async_copy(a, b, r.ssem.at[i]) for i, (a, b) in enumerate(pairs)]
    weight = column_copies(r.w0, r.wr, r.wsem)
    for copy in small:
        copy.start()

    @pl.when(first)
    def _():
        run_all(hidden_copies(r, 0, r.send_r))

    for copy in small:
        copy.wait()

    @pl.when(first | second)
    def _():
        for copy in weight:
            copy.start()

    @pl.when(first)
    def _():
        sums, counts = relay_layer(r, r.send_r, 0, r.wr, weight)
        add_stats(r.stats, 0, sums, counts)

    @pl.when(second)
    def _():
        for copy in weight:
            copy.wait()

    @pl.when(jnp.logical_not(first | second))
    def _():
        ids = jnp.concatenate([r.ids[m] for m in range(r.ids.shape[0])], axis=0)
        r.small[0:60, :] = r.router[...]
        r.small[64:124, :] = r.scale[...]
        r.small[128:129, :] = r.gain[...]
        r.small[144:176, 0:64] = ids.astype(jnp.float32).astype(jnp.bfloat16)


def relay_step(t, r, first, second, core):
    cur = r.cur if t >= 2 else r.send_r
    if t < CHUNKS:

        @pl.when(first)
        def _():
            run_all(hidden_copies(r, t, cur))

    if t >= 2:

        @pl.when(second)
        def _():
            cur[...] = r.recv_r[...]

    @pl.when(first if t < 2 else (second if t >= CHUNKS else first | second))
    def _():
        sums, counts = relay_layer(r, cur, t - 2 * core, r.wr)
        add_stats(r.stats, 2 * core, sums, counts)

    if 2 <= t < CHUNKS:

        @pl.when(first)
        def _():
            r.send_r[...] = cur[...]

    if t >= 2:

        @pl.when(second)
        def _():
            r.send_b[...] = cur[0:64, :]
            r.send_a[...] = cur[64:128, :]


def pair_step(t, r, chip, core):
    chunk = t - 2 - 2 * chip
    cur = r.send_b

    @pl.when((chip >= 1) & (chunk >= 0) & (chunk < CHUNKS))
    def _():
        if hasattr(r, "recv_a"):
            from_a = (chip == 1) & (core == 1)

            @pl.when(from_a)
            def _():
                cur[...] = r.recv_a[...]

            @pl.when(jnp.logical_not(from_a))
            def _():
                cur[...] = r.recv_b[...]
        else:
            cur[...] = r.recv_b[...]
        batch = 2 * chunk + core

        def one(layer, carry):
            own = layer == core

            def pick(rows, c, n):
                return jnp.where(own, r.small[rows, c : c + n], r.small2[rows, c : c + n])

            table = pick(slice(144, 176), 0, 64).astype(jnp.float32)
            ids = table[0:4]
            for m in range(1, 8):
                ids = jnp.where(batch == m, table[4 * m : 4 * m + 4], ids)
            sums, counts = front(
                64,
                lambda c, n: cur[:, c : c + n],
                lambda c, n: pick(slice(128, 129), c, n),
                lambda: pick(slice(0, 60), 0, cur.shape[1]),
                lambda c, n: pick(slice(64, 124), c, n),
                ids.astype(jnp.int32),
                r,
            )

            def mix():
                for n in range(0, cur.shape[1], WIDE):
                    mix_block(64, cur, r.mixed, r.w, n, (own, r.w2))

            if t == STEPS - 1:
                pl.when(layer == 0)(mix)
            else:
                mix()
            add_stats(r.stats, 2 * layer, sums, counts)
            return carry

        lax.fori_loop(0, 2, one, 0)


def stats_table(r):
    table = jnp.transpose(
        jnp.concatenate([r.stats[...], jnp.zeros((128 - 60, 128), jnp.float32)], axis=0)
    )
    for layer in range(2):
        row = table[2 * layer : 2 * layer + 1, :]
        counts = table[2 * layer + 1 : 2 * layer + 2, :]
        at = lax.broadcasted_iota(jnp.int32, row.shape, 1)
        row = jnp.where(at < 60, row, jnp.where(at >= 64, pltpu.roll(counts, 64, 1), 0.0))
        r.table[32 * layer : 32 * layer + 32, :] = jnp.broadcast_to(row, (32, 128))


def step_kernel(t, names, *refs):
    r = SimpleNamespace(**dict(zip(names, refs)))
    chip, core = lax.axis_index(X), lax.axis_index(C)
    first, second = (chip == 0) & (core == 0), (chip == 0) & (core == 1)
    if t:
        r.stats[...] = r.stats0[...]
    else:
        r.stats[...] = jnp.zeros_like(r.stats)
        first_step(r, first, second)
    if 0 < t < RELAY_END:
        relay_step(t, r, first, second, core)
    if t >= PAIR_START:
        pair_step(t, r, chip, core)
    if t == STEPS - 1:
        stats_table(r)


def tail_kernel(names, *refs):
    r = SimpleNamespace(**dict(zip(names, refs)))
    chip, core = lax.axis_index(X), lax.axis_index(C)
    for k, part in enumerate((r.part0, r.part1, r.part2)):

        @pl.when(chip == k)
        def _():
            pltpu.make_async_copy(part, r.out, r.sem).start()

    for own, source in ((1, r.w0), (0, r.w1)):

        @pl.when((chip == CHIPS - 1) & (core == own))
        def _():
            for copy in column_copies(source, r.w, r.wsem):
                copy.start()

    @pl.when(chip == CHIPS - 1)
    def _():
        r.cur[...] = r.mid[...]
        for i, copy in enumerate(column_copies(r.w0, r.w, r.wsem)):
            copy.wait()
            mix_block(64, r.cur, r.mixed, r.w, i * WIDE)
        pltpu.make_async_copy(r.cur, r.out, r.sem).start()

    pltpu.make_async_copy(r.cur, r.out, r.sem).wait()


def loss_kernel(token_total, arrived, balance):
    total = jnp.sum(arrived[...], axis=0, keepdims=True)
    counts = pltpu.roll(total, 64, 1)
    at = lax.broadcasted_iota(jnp.int32, total.shape, 1)
    terms = jnp.where(at < 60, (counts / (token_total * 4.0)) * (total / token_total), 0.0)
    balance[0] = 60.0 * jnp.sum(terms)


def call(kernel, ins, outs, scratch, hbm=(), space=pltpu.VMEM):
    spaces = [pltpu.HBM if n in hbm else pltpu.VMEM for n in ins]
    args = [pltpu.with_memory_space_constraint(v, m) for v, m in zip(ins.values(), spaces)]
    got = pl.pallas_call(
        kernel,
        out_shape=[space(*v) for v in outs.values()],
        in_specs=[pl.BlockSpec(memory_space=m) for m in spaces],
        out_specs=[pl.BlockSpec(memory_space=space) for _ in outs],
        scratch_shapes=list(scratch.values()),
        compiler_params=pltpu.CompilerParams(vmem_limit_bytes=VMEM_LIMIT),
        cost_estimate=pl.CostEstimate(
            flops=2 * 64 * 2048 * 2048 * 2, bytes_accessed=8 * 1024 * 1024, transcendentals=0
        ),
    )(*args)
    return SimpleNamespace(**dict(zip(outs, got)))


R_HOPS = range(CHUNKS)
A_HOPS = range(2, RELAY_END)
B_HOPS = range(2, STEPS - 1)


def run_step(t, ins, outs):
    rows = 128 if t < RELAY_END else 64
    scratch = dict(
        nrm=pltpu.VMEM((rows, 2048), jnp.float32), nbf=pltpu.VMEM((rows, 2048), jnp.bfloat16)
    )
    if t < STEPS - 1:
        scratch |= dict(mixed=pltpu.VMEM((rows, 2048), jnp.bfloat16))
    else:
        scratch |= dict(stats=pltpu.VMEM((60, 128), jnp.float32))
    if 2 <= t < RELAY_END:
        scratch |= dict(cur=pltpu.VMEM((128, 2048), jnp.bfloat16))
    if t < CHUNKS:
        scratch |= dict(xsem=pltpu.SemaphoreType.DMA((2,)))
    if t == 0:
        scratch |= dict(wsem=pltpu.SemaphoreType.DMA((4,)), ssem=pltpu.SemaphoreType.DMA((4,)))
    kernel = functools.partial(step_kernel, t, (*ins, *outs, *scratch))
    hbm = tuple(dict(hidden=0, w0=0, router0=0, scale0=0, gain0=0, ids0=0))
    return call(kernel, ins, outs, scratch, hbm)


def hop_pairs(t):
    pairs = [(1, 2)] if t in A_HOPS else []
    for chip in (1, 2, 3):
        chunk = t - 2 - 2 * chip
        if 0 <= chunk < CHUNKS:
            goal = chip + 1 if chip < CHIPS - 1 else chunk
            pairs += [(2 * chip + c, 2 * goal + c) for c in range(2)]
    return pairs


def per_device(hidden_in, norm_gain, router_weight, expert_scale, mix_weight, routes):
    batches, rows, width = hidden_in.shape
    experts = router_weight.shape[2]
    router = jnp.transpose(router_weight[0])
    ids = jnp.transpose(routes[0], (0, 2, 1))
    scale, w = expert_scale[0], mix_weight[0]
    swap = [(2 * x + c, 2 * x + 1 - c) for x in range(1, CHIPS) for c in range(2)]

    def hop(x, pairs):
        return lax.ppermute(x, SEC, pairs)

    half = ((rows, width), jnp.bfloat16)
    full = ((2 * rows, width), jnp.bfloat16)
    sums = dict(stats=((experts, 128), jnp.float32))

    def like(x):
        return (x.shape, x.dtype)

    w2 = hop(w, swap)
    got = run_step(
        0,
        dict(hidden=hidden_in, w0=w, router0=router, scale0=scale, gain0=norm_gain, ids0=ids),
        dict(
            wr=like(w),
            router=like(router),
            scale=like(scale),
            gain=like(norm_gain),
            ids=like(ids),
            send_r=full,
            small=((176, width), jnp.bfloat16),
        )
        | sums,
    )
    relay = dict(wr=got.wr, router=got.router, scale=got.scale, gain=got.gain, ids=got.ids)
    hop_r, hop_a, hop_b = {0: hop(got.send_r, [(0, 1)])}, {}, {}
    small2 = hop(got.small, swap)
    pair = dict(small=got.small, small2=small2, w=w, w2=w2)
    for t in range(1, STEPS):
        ins, outs = dict(stats0=got.stats), dict(sums)
        if t < RELAY_END:
            ins |= relay
        if t < CHUNKS:
            ins |= dict(hidden=hidden_in)
            outs |= dict(send_r=full)
        if t in A_HOPS:
            ins |= dict(recv_r=hop_r[t - 2])
            outs |= dict(send_a=half)
        if t >= 2:
            outs |= dict(send_b=half)
        if t >= PAIR_START:
            ins |= pair | dict(recv_b=hop_b[t - 2])
            if t - 2 in A_HOPS:
                ins |= dict(recv_a=hop_a[t - 2])
        if t == STEPS - 1:
            outs = dict(send_b=half, mixed=half, table=((2 * 32, 128), jnp.float32))
        got = run_step(t, ins, outs)
        if t in B_HOPS:
            hop_b[t] = hop(got.send_b, hop_pairs(t))
        if t in A_HOPS:
            hop_a[t] = hop(got.send_a, [(1, 3)])
        if t in R_HOPS:
            hop_r[t] = hop(got.send_r, [(0, 1)])
    arrived = lax.all_to_all(got.table, (C, Z, Y), 0, 0, tiled=True)
    ins = dict(part0=hop_b[8], part1=hop_b[9], part2=hop_b[10])
    ins |= dict(mid=got.send_b, mixed=got.mixed, w0=w, w1=w2)
    scratch = dict(
        cur=pltpu.VMEM(*half),
        w=pltpu.VMEM(w.shape, w.dtype),
        sem=pltpu.SemaphoreType.DMA,
        wsem=pltpu.SemaphoreType.DMA((4,)),
    )
    kernel = functools.partial(tail_kernel, (*ins, *dict(out=0), *scratch))
    hbm = tuple(dict(w0=0, w1=0))
    out = call(kernel, ins, dict(out=half), scratch, hbm, pltpu.HBM).out
    token_total = float(batches * rows * lax.axis_size(Z) * lax.axis_size(Y))
    kernel = functools.partial(loss_kernel, token_total)
    outs = dict(balance=((1,), jnp.float32))
    loss = call(kernel, dict(arrived=arrived), outs, {}, (), pltpu.SMEM)
    return out[None], loss.balance


def solution(mesh):
    torus = Mesh(mesh.devices.reshape(CHIPS, 2, 8, 4), (X, C, Z, Y))
    dp = (Z, Y)

    return jax.shard_map(
        per_device,
        mesh=torus,
        in_specs=(
            P(None, dp, None),
            P(SEC, None),
            P(SEC, None, None),
            P(SEC, None, None),
            P(SEC, None, None),
            P(SEC, None, dp, None),
        ),
        out_specs=(P(SEC, dp, None), P(SEC)),
        check_vma=False,
    )
```

```python
import functools
from types import SimpleNamespace

import jax
import jax.numpy as jnp
from jax import lax
from jax.experimental import pallas as pl
from jax.experimental.pallas import tpu as pltpu
from jax.sharding import Mesh
from jax.sharding import PartitionSpec as P


X, C, Z, Y = "xczy"
SEC = (X, C)
CHIPS = 4
CHUNKS = 4
RELAY_END = 6
PAIR_START = 4
STEPS = 12
COLS = 256
WIDE = 512
VMEM_LIMIT = 12 * 1024 * 1024


def front(rows, load_x, load_gain, load_router, load_scale, ids, r):
    width = r.nrm.shape[1]
    acc = None
    for c in range(0, width, COLS):
        xs = load_x(c, COLS).astype(jnp.float32)
        acc = xs * xs if acc is None else acc + xs * xs
    mean_square = jnp.sum(acc, axis=-1, keepdims=True) * jnp.float32(1.0 / width)
    inv = lax.rsqrt(mean_square + 1e-06)
    for c in range(0, width, COLS):
        xs = load_x(c, COLS).astype(jnp.float32)
        normed = xs * inv * load_gain(c, COLS).astype(jnp.float32)
        r.nrm[0:rows, c : c + COLS] = normed
        r.nbf[0:rows, c : c + COLS] = normed.astype(jnp.bfloat16)
    logits = lax.dot_general(
        load_router(),
        r.nbf[0:rows, :],
        (((1,), (1,)), ((), ())),
        preferred_element_type=jnp.float32,
    )
    exponent = jnp.exp(logits)
    probs = exponent / jnp.sum(exponent, axis=0, keepdims=True)
    expert = lax.broadcasted_iota(jnp.int32, probs.shape, 0)
    hit = ids[0:1, :] == expert
    for k in range(1, ids.shape[0]):
        hit = hit | (ids[k : k + 1, :] == expert)
    chosen = jnp.where(hit, 1.0, 0.0).astype(jnp.float32)
    gates = jnp.transpose(probs * chosen).astype(jnp.bfloat16)
    for c in range(0, width, COLS):
        channel = jnp.dot(gates, load_scale(c, COLS), preferred_element_type=jnp.float32)
        r.mixed[0:rows, c : c + COLS] = (r.nrm[0:rows, c : c + COLS] * channel).astype(
            jnp.bfloat16
        )
    return (
        jnp.sum(probs, axis=1, keepdims=True),
        jnp.sum(chosen, axis=1, keepdims=True),
    )


def add_update(rows, cur, n, update):
    cur[0:rows, n : n + WIDE] = (cur[0:rows, n : n + WIDE].astype(jnp.float32) + update).astype(
        jnp.bfloat16
    )


def mix_block(rows, cur, mixed, w, n):
    weight = w[:, n : n + WIDE]
    update = jnp.dot(mixed[0:rows, :], weight, preferred_element_type=jnp.float32)
    add_update(rows, cur, n, update)


def mix_all(rows, cur, mixed, load_w):
    width = cur.shape[1]
    blocks = range(0, width, WIDE)
    sums = {n: None for n in blocks}
    for k in range(0, width, COLS):
        for n in blocks:
            part = jnp.dot(
                mixed[0:rows, k : k + COLS],
                load_w(slice(k, k + COLS), slice(n, n + WIDE)),
                preferred_element_type=jnp.float32,
            )
            sums[n] = part if k == 0 else sums[n] + part
    for n in blocks:
        add_update(rows, cur, n, sums[n])


def add_stats(stats, lane, sums, counts):
    at = lax.broadcasted_iota(jnp.int32, stats.shape, 1)
    stats[...] += jnp.where(at == lane, sums, 0.0) + jnp.where(at == lane + 1, counts, 0.0)


def relay_layer(r, cur, chunk, weight, waits=None):
    rows = cur.shape[0]
    sums, counts = front(
        rows,
        lambda c, n: cur[0:rows, c : c + n],
        lambda c, n: r.gain[:, c : c + n],
        lambda: r.router[...],
        lambda c, n: r.scale[:, c : c + n],
        jnp.concatenate([r.ids[2 * chunk], r.ids[2 * chunk + 1]], axis=1),
        r,
    )
    if waits is None:
        mix_all(rows, cur, r.mixed, lambda k, n: weight[k, n])
        return sums, counts
    for i, n in enumerate(range(0, cur.shape[1], WIDE)):
        waits[i].wait()
        mix_block(rows, cur, r.mixed, weight, n)
    return sums, counts


def column_copies(source, to, sems):
    return [
        pltpu.make_async_copy(source.at[:, pl.ds(n, WIDE)], to.at[:, pl.ds(n, WIDE)], sems.at[i])
        for i, n in enumerate(range(0, to.shape[1], WIDE))
    ]


def run_all(copies):
    for copy in copies:
        copy.start()
    for copy in copies:
        copy.wait()


def hidden_copies(r, chunk, to):
    return [
        pltpu.make_async_copy(r.hidden.at[2 * chunk + b], to.at[pl.ds(64 * b, 64)], r.xsem.at[b])
        for b in range(2)
    ]


def first_step(r, first, second):
    pairs = ((r.gain0, r.gain), (r.ids0, r.ids), (r.router0, r.router), (r.scale0, r.scale))
    small = [pltpu.make_async_copy(a, b, r.ssem.at[i]) for i, (a, b) in enumerate(pairs)]
    weight = column_copies(r.w0, r.wr, r.wsem)
    for copy in small:
        copy.start()

    @pl.when(first)
    def _():
        for copy in hidden_copies(r, 0, r.send_r):
            copy.start()

    @pl.when(first | second)
    def _():
        weight[0].start()

    for copy in small:
        copy.wait()

    @pl.when(first)
    def _():
        for copy in hidden_copies(r, 0, r.send_r):
            copy.wait()

    @pl.when(first | second)
    def _():
        for copy in weight[1:]:
            copy.start()

    @pl.when(first)
    def _():
        sums, counts = relay_layer(r, r.send_r, 0, r.wr, weight)
        add_stats(r.stats, 0, sums, counts)

    @pl.when(second)
    def _():
        for copy in weight:
            copy.wait()

    @pl.when(jnp.logical_not(first | second))
    def _():
        ids = jnp.concatenate([r.ids[m] for m in range(r.ids.shape[0])], axis=0)
        r.small[0:60, :] = r.router[...]
        r.small[64:124, :] = r.scale[...]
        r.small[128:129, :] = r.gain[...]
        r.small[144:176, 0:64] = ids.astype(jnp.float32).astype(jnp.bfloat16)


def relay_step(t, r, first, second, core):
    cur = r.cur if t >= 2 else r.send_r
    if t < CHUNKS:

        @pl.when(first)
        def _():
            run_all(hidden_copies(r, t, cur))

    if t >= 2:

        @pl.when(second)
        def _():
            cur[...] = r.recv_r[...]

    @pl.when(first if t < 2 else (second if t >= CHUNKS else first | second))
    def _():
        sums, counts = relay_layer(r, cur, t - 2 * core, r.wr)
        add_stats(r.stats, 2 * core, sums, counts)

    if 2 <= t < CHUNKS:

        @pl.when(first)
        def _():
            r.send_r[...] = cur[...]

    if t >= 2:

        @pl.when(second)
        def _():
            r.send_a[...] = cur[0:64, :]
            r.send_b[...] = cur[64:128, :]


def pair_step(t, r, chip, core):
    chunk = t - 2 - 2 * chip
    cur = r.send_b

    @pl.when((chip >= 1) & (chunk >= 0) & (chunk < CHUNKS))
    def _():
        if hasattr(r, "recv_a"):
            from_a = (chip == 1) & (core == 0)

            @pl.when(from_a)
            def _():
                cur[...] = r.recv_a[...]

            @pl.when(jnp.logical_not(from_a))
            def _():
                cur[...] = r.recv_b[...]
        else:
            cur[...] = r.recv_b[...]
        batch = 2 * chunk + core

        def one(layer, carry):
            own = layer == core

            def pick(rows, c, n):
                return jnp.where(own, r.small[rows, c : c + n], r.small2[rows, c : c + n])

            table = pick(slice(144, 176), 0, 64).astype(jnp.float32)
            ids = table[0:4]
            for m in range(1, 8):
                ids = jnp.where(batch == m, table[4 * m : 4 * m + 4], ids)
            sums, counts = front(
                64,
                lambda c, n: cur[:, c : c + n],
                lambda c, n: pick(slice(128, 129), c, n),
                lambda: pick(slice(0, 60), 0, cur.shape[1]),
                lambda c, n: pick(slice(64, 124), c, n),
                ids.astype(jnp.int32),
                r,
            )

            def mix():
                mix_all(64, cur, r.mixed, lambda k, n: jnp.where(own, r.w[k, n], r.w2[k, n]))

            if t == STEPS - 1:
                pl.when(layer == 0)(mix)
            else:
                mix()
            add_stats(r.stats, 2 * layer, sums, counts)
            return carry

        lax.fori_loop(0, 2, one, 0)


def stats_table(r):
    table = jnp.transpose(
        jnp.concatenate([r.stats[...], jnp.zeros((128 - 60, 128), jnp.float32)], axis=0)
    )
    for layer in range(2):
        row = table[2 * layer : 2 * layer + 1, :]
        counts = table[2 * layer + 1 : 2 * layer + 2, :]
        at = lax.broadcasted_iota(jnp.int32, row.shape, 1)
        row = jnp.where(at < 60, row, jnp.where(at >= 64, pltpu.roll(counts, 64, 1), 0.0))
        r.table[32 * layer : 32 * layer + 32, :] = jnp.broadcast_to(row, (32, 128))


def step_kernel(t, names, *refs):
    r = SimpleNamespace(**dict(zip(names, refs)))
    chip, core = lax.axis_index(X), lax.axis_index(C)
    first, second = (chip == 0) & (core == 0), (chip == 0) & (core == 1)
    if t:
        r.stats[...] = r.stats0[...]
    else:
        r.stats[...] = jnp.zeros_like(r.stats)
        first_step(r, first, second)
    if 0 < t < RELAY_END:
        relay_step(t, r, first, second, core)
    if t >= PAIR_START:
        pair_step(t, r, chip, core)
    if t == STEPS - 1:
        stats_table(r)


def tail_kernel(names, *refs):
    r = SimpleNamespace(**dict(zip(names, refs)))
    chip, core = lax.axis_index(X), lax.axis_index(C)
    for k, part in enumerate((r.part0, r.part1, r.part2)):

        @pl.when(chip == k)
        def _():
            pltpu.make_async_copy(part, r.out, r.sem).start()

    for own, source in ((1, r.w0), (0, r.w1)):

        @pl.when((chip == CHIPS - 1) & (core == own))
        def _():
            for copy in column_copies(source, r.w, r.wsem):
                copy.start()

    @pl.when(chip == CHIPS - 1)
    def _():
        r.cur[...] = r.mid[...]
        for i, copy in enumerate(column_copies(r.w0, r.w, r.wsem)):
            copy.wait()
            mix_block(64, r.cur, r.mixed, r.w, i * WIDE)
        pltpu.make_async_copy(r.cur, r.out, r.sem).start()

    pltpu.make_async_copy(r.cur, r.out, r.sem).wait()


def loss_kernel(token_total, arrived, balance):
    total = jnp.sum(arrived[...], axis=0, keepdims=True)
    counts = pltpu.roll(total, 64, 1)
    at = lax.broadcasted_iota(jnp.int32, total.shape, 1)
    terms = jnp.where(at < 60, (counts / (token_total * 4.0)) * (total / token_total), 0.0)
    balance[0] = 60.0 * jnp.sum(terms)


def call(kernel, ins, outs, scratch, hbm=(), space=pltpu.VMEM):
    spaces = [pltpu.HBM if n in hbm else pltpu.VMEM for n in ins]
    args = [pltpu.with_memory_space_constraint(v, m) for v, m in zip(ins.values(), spaces)]
    got = pl.pallas_call(
        kernel,
        out_shape=[space(*v) for v in outs.values()],
        in_specs=[pl.BlockSpec(memory_space=m) for m in spaces],
        out_specs=[pl.BlockSpec(memory_space=space) for _ in outs],
        scratch_shapes=list(scratch.values()),
        compiler_params=pltpu.CompilerParams(vmem_limit_bytes=VMEM_LIMIT),
        cost_estimate=pl.CostEstimate(
            flops=2 * 64 * 2048 * 2048 * 2, bytes_accessed=8 * 1024 * 1024, transcendentals=0
        ),
    )(*args)
    return SimpleNamespace(**dict(zip(outs, got)))


R_HOPS = range(CHUNKS)
A_HOPS = range(2, RELAY_END)
B_HOPS = range(2, STEPS - 1)


def run_step(t, ins, outs):
    rows = 128 if t < RELAY_END else 64
    scratch = dict(
        nrm=pltpu.VMEM((rows, 2048), jnp.float32), nbf=pltpu.VMEM((rows, 2048), jnp.bfloat16)
    )
    if t < STEPS - 1:
        scratch |= dict(mixed=pltpu.VMEM((rows, 2048), jnp.bfloat16))
    else:
        scratch |= dict(stats=pltpu.VMEM((60, 128), jnp.float32))
    if 2 <= t < RELAY_END:
        scratch |= dict(cur=pltpu.VMEM((128, 2048), jnp.bfloat16))
    if t < CHUNKS:
        scratch |= dict(xsem=pltpu.SemaphoreType.DMA((2,)))
    if t == 0:
        scratch |= dict(wsem=pltpu.SemaphoreType.DMA((4,)), ssem=pltpu.SemaphoreType.DMA((4,)))
    kernel = functools.partial(step_kernel, t, (*ins, *outs, *scratch))
    hbm = tuple(dict(hidden=0, w0=0, router0=0, scale0=0, gain0=0, ids0=0))
    return call(kernel, ins, outs, scratch, hbm)


def hop_pairs(t):
    pairs = [(1, 3)] if t in A_HOPS else []
    for chip in (1, 2, 3):
        chunk = t - 2 - 2 * chip
        if 0 <= chunk < CHUNKS:
            goal = chip + 1 if chip < CHIPS - 1 else chunk
            pairs += [(2 * chip + c, 2 * goal + c) for c in range(2)]
    return pairs


def per_device(hidden_in, norm_gain, router_weight, expert_scale, mix_weight, routes):
    batches, rows, width = hidden_in.shape
    experts = router_weight.shape[2]
    router = jnp.transpose(router_weight[0])
    ids = jnp.transpose(routes[0], (0, 2, 1))
    scale, w = expert_scale[0], mix_weight[0]
    swap = [(2 * x + c, 2 * x + 1 - c) for x in range(1, CHIPS) for c in range(2)]

    def hop(x, pairs):
        return lax.ppermute(x, SEC, pairs)

    half = ((rows, width), jnp.bfloat16)
    full = ((2 * rows, width), jnp.bfloat16)
    sums = dict(stats=((experts, 128), jnp.float32))

    def like(x):
        return (x.shape, x.dtype)

    w2 = hop(w, swap)
    got = run_step(
        0,
        dict(hidden=hidden_in, w0=w, router0=router, scale0=scale, gain0=norm_gain, ids0=ids),
        dict(
            wr=like(w),
            router=like(router),
            scale=like(scale),
            gain=like(norm_gain),
            ids=like(ids),
            send_r=full,
            small=((176, width), jnp.bfloat16),
        )
        | sums,
    )
    relay = dict(wr=got.wr, router=got.router, scale=got.scale, gain=got.gain, ids=got.ids)
    hop_r, hop_a, hop_b = {0: hop(got.send_r, [(0, 1)])}, {}, {}
    small2 = hop(got.small, swap)
    pair = dict(small=got.small, small2=small2, w=w, w2=w2)
    for t in range(1, STEPS):
        ins, outs = dict(stats0=got.stats), dict(sums)
        if t < RELAY_END:
            ins |= relay
        if t < CHUNKS:
            ins |= dict(hidden=hidden_in)
            outs |= dict(send_r=full)
        if t in A_HOPS:
            ins |= dict(recv_r=hop_r[t - 2])
            outs |= dict(send_a=half)
        if t >= 2:
            outs |= dict(send_b=half)
        if t >= PAIR_START:
            ins |= pair | dict(recv_b=hop_b[t - 2])
            if t - 2 in A_HOPS:
                ins |= dict(recv_a=hop_a[t - 2])
        if t == STEPS - 1:
            outs = dict(send_b=half, mixed=half, table=((2 * 32, 128), jnp.float32))
        got = run_step(t, ins, outs)
        if t in B_HOPS:
            hop_b[t] = hop(got.send_b, hop_pairs(t))
        if t in A_HOPS:
            hop_a[t] = hop(got.send_a, [(1, 2)])
        if t in R_HOPS:
            hop_r[t] = hop(got.send_r, [(0, 1)])
    arrived = lax.all_to_all(got.table, (C, Z, Y), 0, 0, tiled=True)
    ins = dict(part0=hop_b[8], part1=hop_b[9], part2=hop_b[10])
    ins |= dict(mid=got.send_b, mixed=got.mixed, w0=w, w1=w2)
    scratch = dict(
        cur=pltpu.VMEM(*half),
        w=pltpu.VMEM(w.shape, w.dtype),
        sem=pltpu.SemaphoreType.DMA,
        wsem=pltpu.SemaphoreType.DMA((4,)),
    )
    kernel = functools.partial(tail_kernel, (*ins, *dict(out=0), *scratch))
    hbm = tuple(dict(w0=0, w1=0))
    out = call(kernel, ins, dict(out=half), scratch, hbm, pltpu.HBM).out
    token_total = float(batches * rows * lax.axis_size(Z) * lax.axis_size(Y))
    kernel = functools.partial(loss_kernel, token_total)
    outs = dict(balance=((1,), jnp.float32))
    loss = call(kernel, dict(arrived=arrived), outs, {}, (), pltpu.SMEM)
    return out[None], loss.balance


def solution(mesh):
    torus = Mesh(mesh.devices.reshape(CHIPS, 2, 8, 4), (X, C, Z, Y))
    dp = (Z, Y)

    return jax.shard_map(
        per_device,
        mesh=torus,
        in_specs=(
            P(None, dp, None),
            P(SEC, None),
            P(SEC, None, None),
            P(SEC, None, None),
            P(SEC, None, None),
            P(SEC, None, dp, None),
        ),
        out_specs=(P(SEC, dp, None), P(SEC)),
        check_vma=False,
    )
```

```python
import functools
from types import SimpleNamespace

import jax
import jax.numpy as jnp
from jax import lax
from jax.experimental import pallas as pl
from jax.experimental.pallas import tpu as pltpu
from jax.sharding import Mesh
from jax.sharding import PartitionSpec as P


X, C, Z, Y = "xczy"
SEC = (X, C)
CHIPS = 4
CHUNKS = 4
RELAY_END = 6
PAIR_START = 4
STEPS = 12
COLS = 256
WIDE = 512
VMEM_LIMIT = 12 * 1024 * 1024


def front(rows, load_x, load_gain, load_router, load_scale, ids, r):
    width = r.nrm.shape[1]
    acc = None
    for c in range(0, width, COLS):
        xs = load_x(c, COLS).astype(jnp.float32)
        acc = xs * xs if acc is None else acc + xs * xs
    mean_square = jnp.sum(acc, axis=-1, keepdims=True) * jnp.float32(1.0 / width)
    inv = lax.rsqrt(mean_square + 1e-06)
    for c in range(0, width, COLS):
        xs = load_x(c, COLS).astype(jnp.float32)
        normed = xs * inv * load_gain(c, COLS).astype(jnp.float32)
        r.nrm[0:rows, c : c + COLS] = normed
        r.nbf[0:rows, c : c + COLS] = normed.astype(jnp.bfloat16)
    logits = lax.dot_general(
        load_router(),
        r.nbf[0:rows, :],
        (((1,), (1,)), ((), ())),
        preferred_element_type=jnp.float32,
    )
    exponent = jnp.exp(logits)
    probs = exponent / jnp.sum(exponent, axis=0, keepdims=True)
    expert = lax.broadcasted_iota(jnp.int32, probs.shape, 0)
    hit = ids[0:1, :] == expert
    for k in range(1, ids.shape[0]):
        hit = hit | (ids[k : k + 1, :] == expert)
    chosen = jnp.where(hit, 1.0, 0.0).astype(jnp.float32)
    gates = jnp.transpose(probs * chosen).astype(jnp.bfloat16)
    for c in range(0, width, COLS):
        channel = jnp.dot(gates, load_scale(c, COLS), preferred_element_type=jnp.float32)
        r.mixed[0:rows, c : c + COLS] = (r.nrm[0:rows, c : c + COLS] * channel).astype(
            jnp.bfloat16
        )
    return (
        jnp.sum(probs, axis=1, keepdims=True),
        jnp.sum(chosen, axis=1, keepdims=True),
    )


def add_update(rows, cur, n, update):
    cur[0:rows, n : n + WIDE] = (cur[0:rows, n : n + WIDE].astype(jnp.float32) + update).astype(
        jnp.bfloat16
    )


def mix_block(rows, cur, mixed, w, n):
    weight = w[:, n : n + WIDE]
    update = jnp.dot(mixed[0:rows, :], weight, preferred_element_type=jnp.float32)
    add_update(rows, cur, n, update)


def mix_all(rows, cur, mixed, load_w):
    width = cur.shape[1]
    blocks = range(0, width, WIDE)
    sums = {n: None for n in blocks}
    for k in range(0, width, COLS):
        for n in blocks:
            part = jnp.dot(
                mixed[0:rows, k : k + COLS],
                load_w(slice(k, k + COLS), slice(n, n + WIDE)),
                preferred_element_type=jnp.float32,
            )
            sums[n] = part if k == 0 else sums[n] + part
    for n in blocks:
        add_update(rows, cur, n, sums[n])


def add_stats(stats, lane, sums, counts):
    at = lax.broadcasted_iota(jnp.int32, stats.shape, 1)
    stats[...] += jnp.where(at == lane, sums, 0.0) + jnp.where(at == lane + 1, counts, 0.0)


def relay_layer(r, cur, chunk, weight, waits=None):
    rows = cur.shape[0]
    sums, counts = front(
        rows,
        lambda c, n: cur[0:rows, c : c + n],
        lambda c, n: r.gain[:, c : c + n],
        lambda: r.router[...],
        lambda c, n: r.scale[:, c : c + n],
        jnp.concatenate([r.ids[2 * chunk], r.ids[2 * chunk + 1]], axis=1),
        r,
    )
    if waits is None:
        mix_all(rows, cur, r.mixed, lambda k, n: weight[k, n])
        return sums, counts
    for i, n in enumerate(range(0, cur.shape[1], WIDE)):
        waits[i].wait()
        mix_block(rows, cur, r.mixed, weight, n)
    return sums, counts


def column_copies(source, to, sems):
    return [
        pltpu.make_async_copy(source.at[:, pl.ds(n, WIDE)], to.at[:, pl.ds(n, WIDE)], sems.at[i])
        for i, n in enumerate(range(0, to.shape[1], WIDE))
    ]


def run_all(copies):
    for copy in copies:
        copy.start()
    for copy in copies:
        copy.wait()


def hidden_copies(r, chunk, to):
    return [
        pltpu.make_async_copy(r.hidden.at[2 * chunk + b], to.at[pl.ds(64 * b, 64)], r.xsem.at[b])
        for b in range(2)
    ]


def first_step(r, first, second):
    pairs = ((r.gain0, r.gain), (r.ids0, r.ids), (r.router0, r.router), (r.scale0, r.scale))
    small = [pltpu.make_async_copy(a, b, r.ssem.at[i]) for i, (a, b) in enumerate(pairs)]
    weight = column_copies(r.w0, r.wr, r.wsem)
    for copy in small:
        copy.start()

    @pl.when(first)
    def _():
        for copy in hidden_copies(r, 0, r.send_r):
            copy.start()

    @pl.when(first | second)
    def _():
        weight[0].start()

    for copy in small:
        copy.wait()

    @pl.when(first)
    def _():
        for copy in hidden_copies(r, 0, r.send_r):
            copy.wait()

    @pl.when(first | second)
    def _():
        for copy in weight[1:]:
            copy.start()

    @pl.when(first)
    def _():
        sums, counts = relay_layer(r, r.send_r, 0, r.wr, weight)
        add_stats(r.stats, 0, sums, counts)

    @pl.when(second)
    def _():
        for copy in weight:
            copy.wait()

    @pl.when(jnp.logical_not(first | second))
    def _():
        ids = jnp.concatenate([r.ids[m] for m in range(r.ids.shape[0])], axis=0)
        r.small[0:60, :] = r.router[...]
        r.small[64:124, :] = r.scale[...]
        r.small[128:129, :] = r.gain[...]
        r.small[144:176, 0:64] = ids.astype(jnp.float32).astype(jnp.bfloat16)


def relay_step(t, r, first, second, core):
    cur = r.cur if t >= 2 else r.send_r
    if t < CHUNKS:

        @pl.when(first)
        def _():
            run_all(hidden_copies(r, t, cur))

    if t >= 2:

        @pl.when(second)
        def _():
            cur[...] = r.recv_r[...]

    @pl.when(first if t < 2 else (second if t >= CHUNKS else first | second))
    def _():
        sums, counts = relay_layer(r, cur, t - 2 * core, r.wr)
        add_stats(r.stats, 2 * core, sums, counts)

    if 2 <= t < CHUNKS:

        @pl.when(first)
        def _():
            r.send_r[...] = cur[...]

    if t >= 2:

        @pl.when(second)
        def _():
            r.send_a[...] = cur[0:64, :]
            r.send_b[...] = cur[64:128, :]


def pair_step(t, r, chip, core):
    chunk = t - 2 - 2 * chip
    cur = r.send_b

    @pl.when((chip >= 1) & (chunk >= 0) & (chunk < CHUNKS))
    def _():
        if hasattr(r, "recv_a"):
            from_a = (chip == 1) & (core == 0)

            @pl.when(from_a)
            def _():
                cur[...] = r.recv_a[...]

            @pl.when(jnp.logical_not(from_a))
            def _():
                cur[...] = r.recv_b[...]
        else:
            cur[...] = r.recv_b[...]
        batch = 2 * chunk + jnp.where(chip == 2, 1 - core, core)

        def one(layer, carry):
            own = layer == core

            def pick(rows, c, n):
                return jnp.where(own, r.small[rows, c : c + n], r.small2[rows, c : c + n])

            table = pick(slice(144, 176), 0, 64).astype(jnp.float32)
            ids = table[0:4]
            for m in range(1, 8):
                ids = jnp.where(batch == m, table[4 * m : 4 * m + 4], ids)
            sums, counts = front(
                64,
                lambda c, n: cur[:, c : c + n],
                lambda c, n: pick(slice(128, 129), c, n),
                lambda: pick(slice(0, 60), 0, cur.shape[1]),
                lambda c, n: pick(slice(64, 124), c, n),
                ids.astype(jnp.int32),
                r,
            )

            def mix():
                mix_all(64, cur, r.mixed, lambda k, n: jnp.where(own, r.w[k, n], r.w2[k, n]))

            if t == STEPS - 1:
                pl.when(layer == 0)(mix)
            else:
                mix()
            add_stats(r.stats, 2 * layer, sums, counts)
            return carry

        lax.fori_loop(0, 2, one, 0)


def stats_table(r):
    table = jnp.transpose(
        jnp.concatenate([r.stats[...], jnp.zeros((128 - 60, 128), jnp.float32)], axis=0)
    )
    for layer in range(2):
        row = table[2 * layer : 2 * layer + 1, :]
        counts = table[2 * layer + 1 : 2 * layer + 2, :]
        at = lax.broadcasted_iota(jnp.int32, row.shape, 1)
        row = jnp.where(at < 60, row, jnp.where(at >= 64, pltpu.roll(counts, 64, 1), 0.0))
        r.table[32 * layer : 32 * layer + 32, :] = jnp.broadcast_to(row, (32, 128))


def step_kernel(t, names, *refs):
    r = SimpleNamespace(**dict(zip(names, refs)))
    chip, core = lax.axis_index(X), lax.axis_index(C)
    first, second = (chip == 0) & (core == 0), (chip == 0) & (core == 1)
    if t:
        r.stats[...] = r.stats0[...]
    else:
        r.stats[...] = jnp.zeros_like(r.stats)
        first_step(r, first, second)
    if 0 < t < RELAY_END:
        relay_step(t, r, first, second, core)
    if t >= PAIR_START:
        pair_step(t, r, chip, core)
    if t == STEPS - 1:
        stats_table(r)


def tail_kernel(names, *refs):
    r = SimpleNamespace(**dict(zip(names, refs)))
    chip, core = lax.axis_index(X), lax.axis_index(C)
    for k, part in enumerate((r.part0, r.part1, r.part2)):

        @pl.when(chip == k)
        def _():
            pltpu.make_async_copy(part, r.out, r.sem).start()

    for own, source in ((1, r.w0), (0, r.w1)):

        @pl.when((chip == CHIPS - 1) & (core == own))
        def _():
            for copy in column_copies(source, r.w, r.wsem):
                copy.start()

    @pl.when(chip == CHIPS - 1)
    def _():
        r.cur[...] = r.mid[...]
        for i, copy in enumerate(column_copies(r.w0, r.w, r.wsem)):
            copy.wait()
            mix_block(64, r.cur, r.mixed, r.w, i * WIDE)
        pltpu.make_async_copy(r.cur, r.out, r.sem).start()

    pltpu.make_async_copy(r.cur, r.out, r.sem).wait()


def loss_kernel(token_total, arrived, balance):
    total = jnp.sum(arrived[...], axis=0, keepdims=True)
    counts = pltpu.roll(total, 64, 1)
    at = lax.broadcasted_iota(jnp.int32, total.shape, 1)
    terms = jnp.where(at < 60, (counts / (token_total * 4.0)) * (total / token_total), 0.0)
    balance[0] = 60.0 * jnp.sum(terms)


def call(kernel, ins, outs, scratch, hbm=(), space=pltpu.VMEM):
    spaces = [pltpu.HBM if n in hbm else pltpu.VMEM for n in ins]
    args = [pltpu.with_memory_space_constraint(v, m) for v, m in zip(ins.values(), spaces)]
    got = pl.pallas_call(
        kernel,
        out_shape=[space(*v) for v in outs.values()],
        in_specs=[pl.BlockSpec(memory_space=m) for m in spaces],
        out_specs=[pl.BlockSpec(memory_space=space) for _ in outs],
        scratch_shapes=list(scratch.values()),
        compiler_params=pltpu.CompilerParams(vmem_limit_bytes=VMEM_LIMIT),
        cost_estimate=pl.CostEstimate(
            flops=2 * 64 * 2048 * 2048 * 2, bytes_accessed=8 * 1024 * 1024, transcendentals=0
        ),
    )(*args)
    return SimpleNamespace(**dict(zip(outs, got)))


R_HOPS = range(CHUNKS)
A_HOPS = range(2, RELAY_END)
B_HOPS = range(2, STEPS - 1)


def run_step(t, ins, outs):
    rows = 128 if t < RELAY_END else 64
    scratch = dict(
        nrm=pltpu.VMEM((rows, 2048), jnp.float32), nbf=pltpu.VMEM((rows, 2048), jnp.bfloat16)
    )
    if t < STEPS - 1:
        scratch |= dict(mixed=pltpu.VMEM((rows, 2048), jnp.bfloat16))
    else:
        scratch |= dict(stats=pltpu.VMEM((60, 128), jnp.float32))
    if 2 <= t < RELAY_END:
        scratch |= dict(cur=pltpu.VMEM((128, 2048), jnp.bfloat16))
    if t < CHUNKS:
        scratch |= dict(xsem=pltpu.SemaphoreType.DMA((2,)))
    if t == 0:
        scratch |= dict(wsem=pltpu.SemaphoreType.DMA((4,)), ssem=pltpu.SemaphoreType.DMA((4,)))
    kernel = functools.partial(step_kernel, t, (*ins, *outs, *scratch))
    hbm = tuple(dict(hidden=0, w0=0, router0=0, scale0=0, gain0=0, ids0=0))
    return call(kernel, ins, outs, scratch, hbm)


def hop_pairs(t):
    pairs = [(1, 3)] if t in A_HOPS else []
    for chip in (1, 2, 3):
        chunk = t - 2 - 2 * chip
        if 0 <= chunk < CHUNKS:
            if chip < CHIPS - 1:
                pairs += [(2 * chip + c, 2 * (chip + 1) + 1 - c) for c in range(2)]
            else:
                pairs += [(2 * chip + c, 2 * chunk + c) for c in range(2)]
    return pairs


def per_device(hidden_in, norm_gain, router_weight, expert_scale, mix_weight, routes):
    batches, rows, width = hidden_in.shape
    experts = router_weight.shape[2]
    router = jnp.transpose(router_weight[0])
    ids = jnp.transpose(routes[0], (0, 2, 1))
    scale, w = expert_scale[0], mix_weight[0]
    swap = [(2 * x + c, 2 * x + 1 - c) for x in range(1, CHIPS) for c in range(2)]

    def hop(x, pairs):
        return lax.ppermute(x, SEC, pairs)

    half = ((rows, width), jnp.bfloat16)
    full = ((2 * rows, width), jnp.bfloat16)
    sums = dict(stats=((experts, 128), jnp.float32))

    def like(x):
        return (x.shape, x.dtype)

    w2 = hop(w, swap)
    got = run_step(
        0,
        dict(hidden=hidden_in, w0=w, router0=router, scale0=scale, gain0=norm_gain, ids0=ids),
        dict(
            wr=like(w),
            router=like(router),
            scale=like(scale),
            gain=like(norm_gain),
            ids=like(ids),
            send_r=full,
            small=((176, width), jnp.bfloat16),
        )
        | sums,
    )
    relay = dict(wr=got.wr, router=got.router, scale=got.scale, gain=got.gain, ids=got.ids)
    hop_r, hop_a, hop_b = {0: hop(got.send_r, [(0, 1)])}, {}, {}
    small2 = hop(got.small, swap)
    pair = dict(small=got.small, small2=small2, w=w, w2=w2)
    for t in range(1, STEPS):
        ins, outs = dict(stats0=got.stats), dict(sums)
        if t < RELAY_END:
            ins |= relay
        if t < CHUNKS:
            ins |= dict(hidden=hidden_in)
            outs |= dict(send_r=full)
        if t in A_HOPS:
            ins |= dict(recv_r=hop_r[t - 2])
            outs |= dict(send_a=half)
        if t >= 2:
            outs |= dict(send_b=half)
        if t >= PAIR_START:
            ins |= pair | dict(recv_b=hop_b[t - 2])
            if t - 2 in A_HOPS:
                ins |= dict(recv_a=hop_a[t - 2])
        if t == STEPS - 1:
            outs = dict(send_b=half, mixed=half, table=((2 * 32, 128), jnp.float32))
        got = run_step(t, ins, outs)
        if t in B_HOPS:
            hop_b[t] = hop(got.send_b, hop_pairs(t))
        if t in A_HOPS:
            hop_a[t] = hop(got.send_a, [(1, 2)])
        if t in R_HOPS:
            hop_r[t] = hop(got.send_r, [(0, 1)])
    arrived = lax.all_to_all(got.table, (C, Z, Y), 0, 0, tiled=True)
    ins = dict(part0=hop_b[8], part1=hop_b[9], part2=hop_b[10])
    ins |= dict(mid=got.send_b, mixed=got.mixed, w0=w, w1=w2)
    scratch = dict(
        cur=pltpu.VMEM(*half),
        w=pltpu.VMEM(w.shape, w.dtype),
        sem=pltpu.SemaphoreType.DMA,
        wsem=pltpu.SemaphoreType.DMA((4,)),
    )
    kernel = functools.partial(tail_kernel, (*ins, *dict(out=0), *scratch))
    hbm = tuple(dict(w0=0, w1=0))
    out = call(kernel, ins, dict(out=half), scratch, hbm, pltpu.HBM).out
    token_total = float(batches * rows * lax.axis_size(Z) * lax.axis_size(Y))
    kernel = functools.partial(loss_kernel, token_total)
    outs = dict(balance=((1,), jnp.float32))
    loss = call(kernel, dict(arrived=arrived), outs, {}, (), pltpu.SMEM)
    return out[None], loss.balance


def solution(mesh):
    torus = Mesh(mesh.devices.reshape(CHIPS, 2, 8, 4), (X, C, Z, Y))
    dp = (Z, Y)

    return jax.shard_map(
        per_device,
        mesh=torus,
        in_specs=(
            P(None, dp, None),
            P(SEC, None),
            P(SEC, None, None),
            P(SEC, None, None),
            P(SEC, None, None),
            P(SEC, None, dp, None),
        ),
        out_specs=(P(SEC, dp, None), P(SEC)),
        check_vma=False,
    )
```

```python
import functools
from types import SimpleNamespace

import jax
import jax.numpy as jnp
from jax import lax
from jax.experimental import pallas as pl
from jax.experimental.pallas import tpu as pltpu
from jax.sharding import Mesh
from jax.sharding import PartitionSpec as P


X, C, Z, Y = "xczy"
SEC = (X, C)
CHIPS = 4
CHUNKS = 4
RELAY_END = 6
PAIR_START = 4
STEPS = 12
COLS = 256
WIDE = 512
VMEM_LIMIT = 12 * 1024 * 1024


def front(rows, load_x, load_gain, load_router, load_scale, ids, r):
    width = r.nrm.shape[1]
    acc = None
    for c in range(0, width, COLS):
        xs = load_x(c, COLS).astype(jnp.float32)
        acc = xs * xs if acc is None else acc + xs * xs
    mean_square = jnp.sum(acc, axis=-1, keepdims=True) * jnp.float32(1.0 / width)
    inv = lax.rsqrt(mean_square + 1e-06)
    for c in range(0, width, COLS):
        xs = load_x(c, COLS).astype(jnp.float32)
        normed = xs * inv * load_gain(c, COLS).astype(jnp.float32)
        r.nrm[0:rows, c : c + COLS] = normed
        r.nbf[0:rows, c : c + COLS] = normed.astype(jnp.bfloat16)
    logits = lax.dot_general(
        r.nbf[0:rows, :],
        load_router(),
        (((1,), (1,)), ((), ())),
        preferred_element_type=jnp.float32,
    )
    picks = ids.shape[0]
    named = jnp.concatenate([ids.astype(jnp.float32), jnp.zeros((8 - picks, rows))], axis=0)
    named = jnp.transpose(named).astype(jnp.int32)

    def hits(shape, first):
        expert = lax.broadcasted_iota(jnp.int32, shape, 1) - first
        hit = named[:, 0:1] == expert
        for k in range(1, picks):
            hit = hit | (named[:, k : k + 1] == expert)
        return jnp.where(hit, 1.0, 0.0).astype(jnp.float32)

    exponent = jnp.exp(logits)
    probs = exponent / jnp.sum(exponent, axis=1, keepdims=True)
    gates = (probs * hits(probs.shape, 0)).astype(jnp.bfloat16)
    for c in range(0, width, COLS):
        channel = jnp.dot(gates, load_scale(c, COLS), preferred_element_type=jnp.float32)
        r.mixed[0:rows, c : c + COLS] = (r.nrm[0:rows, c : c + COLS] * channel).astype(
            jnp.bfloat16
        )
    return (
        jnp.sum(probs, axis=0, keepdims=True),
        jnp.sum(hits((rows, 128), 64), axis=0, keepdims=True),
    )


def add_update(rows, cur, n, update):
    cur[0:rows, n : n + WIDE] = (cur[0:rows, n : n + WIDE].astype(jnp.float32) + update).astype(
        jnp.bfloat16
    )


def mix_block(rows, cur, mixed, w, n):
    weight = w[:, n : n + WIDE]
    update = jnp.dot(mixed[0:rows, :], weight, preferred_element_type=jnp.float32)
    add_update(rows, cur, n, update)


def mix_all(rows, cur, mixed, load_w):
    width = cur.shape[1]
    blocks = range(0, width, WIDE)
    sums = {n: None for n in blocks}
    for k in range(0, width, COLS):
        for n in blocks:
            part = jnp.dot(
                mixed[0:rows, k : k + COLS],
                load_w(slice(k, k + COLS), slice(n, n + WIDE)),
                preferred_element_type=jnp.float32,
            )
            sums[n] = part if k == 0 else sums[n] + part
    for n in blocks:
        add_update(rows, cur, n, sums[n])


def add_stats(stats, layer, sums, counts):
    stats[pl.ds(layer, 1), :] += counts
    stats[pl.ds(layer, 1), 0 : sums.shape[1]] += sums


def relay_layer(r, cur, chunk, weight, waits=None):
    rows = cur.shape[0]
    sums, counts = front(
        rows,
        lambda c, n: cur[0:rows, c : c + n],
        lambda c, n: r.gain[:, c : c + n],
        lambda: r.router[...],
        lambda c, n: r.scale[:, c : c + n],
        jnp.concatenate([r.ids[2 * chunk], r.ids[2 * chunk + 1]], axis=1),
        r,
    )
    if waits is None:
        mix_all(rows, cur, r.mixed, lambda k, n: weight[k, n])
        return sums, counts
    for i, n in enumerate(range(0, cur.shape[1], WIDE)):
        waits[i].wait()
        mix_block(rows, cur, r.mixed, weight, n)
    return sums, counts


def column_copies(source, to, sems):
    return [
        pltpu.make_async_copy(source.at[:, pl.ds(n, WIDE)], to.at[:, pl.ds(n, WIDE)], sems.at[i])
        for i, n in enumerate(range(0, to.shape[1], WIDE))
    ]


def run_all(copies):
    for copy in copies:
        copy.start()
    for copy in copies:
        copy.wait()


def hidden_copies(r, chunk, to):
    return [
        pltpu.make_async_copy(r.hidden.at[2 * chunk + b], to.at[pl.ds(64 * b, 64)], r.xsem.at[b])
        for b in range(2)
    ]


def first_step(r, first, second):
    pairs = ((r.gain0, r.gain), (r.ids0, r.ids), (r.router0, r.router), (r.scale0, r.scale))
    small = [pltpu.make_async_copy(a, b, r.ssem.at[i]) for i, (a, b) in enumerate(pairs)]
    weight = column_copies(r.w0, r.wr, r.wsem)
    for copy in small:
        copy.start()

    @pl.when(first)
    def _():
        for copy in hidden_copies(r, 0, r.send_r):
            copy.start()

    @pl.when(first | second)
    def _():
        for copy in weight[:2]:
            copy.start()

    for copy in small:
        copy.wait()

    @pl.when(first)
    def _():
        for copy in hidden_copies(r, 0, r.send_r):
            copy.wait()

    @pl.when(first | second)
    def _():
        for copy in weight[2:]:
            copy.start()

    @pl.when(first)
    def _():
        sums, counts = relay_layer(r, r.send_r, 0, r.wr, weight)
        add_stats(r.stats, 0, sums, counts)

    @pl.when(second)
    def _():
        for copy in weight:
            copy.wait()

    @pl.when(jnp.logical_not(first | second))
    def _():
        ids = jnp.concatenate([r.ids[m] for m in range(r.ids.shape[0])], axis=0)
        r.small[0:60, :] = r.router[...]
        r.small[64:124, :] = r.scale[...]
        r.small[128:129, :] = r.gain[...]
        r.small[144:176, 0:64] = ids.astype(jnp.float32).astype(jnp.bfloat16)


def relay_step(t, r, first, second, core):
    cur = r.cur if t >= 2 else r.send_r
    if t < CHUNKS:

        @pl.when(first)
        def _():
            run_all(hidden_copies(r, t, cur))

    if t >= 2:

        @pl.when(second)
        def _():
            cur[...] = r.recv_r[...]

    @pl.when(first if t < 2 else (second if t >= CHUNKS else first | second))
    def _():
        sums, counts = relay_layer(r, cur, t - 2 * core, r.wr)
        add_stats(r.stats, core, sums, counts)

    if 2 <= t < CHUNKS:

        @pl.when(first)
        def _():
            r.send_r[...] = cur[...]

    if t >= 2:

        @pl.when(second)
        def _():
            r.send_a[...] = cur[0:64, :]
            r.send_b[...] = cur[64:128, :]


def pair_step(t, r, chip, core):
    chunk = t - 2 - 2 * chip
    cur = r.send_b

    @pl.when((chip >= 1) & (chunk >= 0) & (chunk < CHUNKS))
    def _():
        if hasattr(r, "recv_a"):
            from_a = (chip == 1) & (core == 0)

            @pl.when(from_a)
            def _():
                cur[...] = r.recv_a[...]

            @pl.when(jnp.logical_not(from_a))
            def _():
                cur[...] = r.recv_b[...]
        else:
            cur[...] = r.recv_b[...]
        batch = 2 * chunk + jnp.where(chip == 2, 1 - core, core)

        def one(layer, carry):
            own = layer == core

            def pick(rows, c, n):
                return jnp.where(own, r.small[rows, c : c + n], r.small2[rows, c : c + n])

            table = pick(slice(144, 176), 0, 64).astype(jnp.float32)
            ids = table[0:4]
            for m in range(1, 8):
                ids = jnp.where(batch == m, table[4 * m : 4 * m + 4], ids)
            sums, counts = front(
                64,
                lambda c, n: cur[:, c : c + n],
                lambda c, n: pick(slice(128, 129), c, n),
                lambda: pick(slice(0, 60), 0, cur.shape[1]),
                lambda c, n: pick(slice(64, 124), c, n),
                ids.astype(jnp.int32),
                r,
            )

            mix_all(64, cur, r.mixed, lambda k, n: jnp.where(own, r.w[k, n], r.w2[k, n]))
            add_stats(r.stats, layer, sums, counts)
            return carry

        lax.fori_loop(0, 2, one, 0)


def step_kernel(t, names, *refs):
    r = SimpleNamespace(**dict(zip(names, refs)))
    chip, core = lax.axis_index(X), lax.axis_index(C)
    first, second = (chip == 0) & (core == 0), (chip == 0) & (core == 1)
    if t:
        r.stats[...] = r.stats0[...]
    else:
        r.stats[...] = jnp.zeros_like(r.stats)
        first_step(r, first, second)
    if 0 < t < RELAY_END:
        relay_step(t, r, first, second, core)
    if t >= PAIR_START:
        pair_step(t, r, chip, core)
    if t == STEPS - 1:
        for layer in range(2):
            row = r.stats[layer : layer + 1, :]
            r.table[32 * layer : 32 * layer + 32, :] = jnp.broadcast_to(row, (32, 128))


def final_kernel(token_total, arrived, part0, part1, part2, last, out, balance, sem):
    chip = lax.axis_index(X)
    for k, part in enumerate((part0, part1, part2, last)):

        @pl.when(chip == k)
        def _():
            pltpu.make_async_copy(part, out, sem).start()

    total = jnp.sum(arrived[...], axis=0, keepdims=True)
    counts = pltpu.roll(total, 64, 1)
    at = lax.broadcasted_iota(jnp.int32, total.shape, 1)
    terms = jnp.where(at < 60, (counts / (token_total * 4.0)) * (total / token_total), 0.0)
    balance[0] = 60.0 * jnp.sum(terms)
    pltpu.make_async_copy(last, out, sem).wait()


def call(kernel, ins, outs, scratch, hbm=(), places=None):
    spaces = [pltpu.HBM if n in hbm else pltpu.VMEM for n in ins]
    args = [pltpu.with_memory_space_constraint(v, m) for v, m in zip(ins.values(), spaces)]
    places = places or [pltpu.VMEM] * len(outs)
    got = pl.pallas_call(
        kernel,
        out_shape=[place(*v) for place, v in zip(places, outs.values())],
        in_specs=[pl.BlockSpec(memory_space=m) for m in spaces],
        out_specs=[pl.BlockSpec(memory_space=place) for place in places],
        scratch_shapes=list(scratch.values()),
        compiler_params=pltpu.CompilerParams(vmem_limit_bytes=VMEM_LIMIT),
        cost_estimate=pl.CostEstimate(
            flops=2 * 64 * 2048 * 2048 * 2, bytes_accessed=8 * 1024 * 1024, transcendentals=0
        ),
    )(*args)
    return SimpleNamespace(**dict(zip(outs, got)))


R_HOPS = range(CHUNKS)
A_HOPS = range(2, RELAY_END)
B_HOPS = range(2, STEPS - 1)


def run_step(t, ins, outs):
    rows = 128 if t < RELAY_END else 64
    scratch = dict(
        nrm=pltpu.VMEM((rows, 2048), jnp.float32), nbf=pltpu.VMEM((rows, 2048), jnp.bfloat16)
    )
    scratch |= dict(mixed=pltpu.VMEM((rows, 2048), jnp.bfloat16))
    if t == STEPS - 1:
        scratch |= dict(stats=pltpu.VMEM((8, 128), jnp.float32))
    if 2 <= t < RELAY_END:
        scratch |= dict(cur=pltpu.VMEM((128, 2048), jnp.bfloat16))
    if t < CHUNKS:
        scratch |= dict(xsem=pltpu.SemaphoreType.DMA((2,)))
    if t == 0:
        scratch |= dict(wsem=pltpu.SemaphoreType.DMA((4,)), ssem=pltpu.SemaphoreType.DMA((4,)))
    kernel = functools.partial(step_kernel, t, (*ins, *outs, *scratch))
    hbm = tuple(dict(hidden=0, w0=0, router0=0, scale0=0, gain0=0, ids0=0))
    return call(kernel, ins, outs, scratch, hbm)


def hop_pairs(t):
    pairs = [(1, 3)] if t in A_HOPS else []
    for chip in (1, 2, 3):
        chunk = t - 2 - 2 * chip
        if 0 <= chunk < CHUNKS:
            if chip < CHIPS - 1:
                pairs += [(2 * chip + c, 2 * (chip + 1) + 1 - c) for c in range(2)]
            else:
                pairs += [(2 * chip + c, 2 * chunk + c) for c in range(2)]
    return pairs


def per_device(hidden_in, norm_gain, router_weight, expert_scale, mix_weight, routes):
    batches, rows, width = hidden_in.shape
    router = jnp.transpose(router_weight[0])
    ids = jnp.transpose(routes[0], (0, 2, 1))
    scale, w = expert_scale[0], mix_weight[0]
    swap = [(2 * x + c, 2 * x + 1 - c) for x in range(1, CHIPS) for c in range(2)]

    def hop(x, pairs):
        return lax.ppermute(x, SEC, pairs)

    half = ((rows, width), jnp.bfloat16)
    full = ((2 * rows, width), jnp.bfloat16)
    sums = dict(stats=((8, 128), jnp.float32))

    def like(x):
        return (x.shape, x.dtype)

    w2 = hop(w, swap)
    got = run_step(
        0,
        dict(hidden=hidden_in, w0=w, router0=router, scale0=scale, gain0=norm_gain, ids0=ids),
        dict(
            wr=like(w),
            router=like(router),
            scale=like(scale),
            gain=like(norm_gain),
            ids=like(ids),
            send_r=full,
            small=((176, width), jnp.bfloat16),
        )
        | sums,
    )
    relay = dict(wr=got.wr, router=got.router, scale=got.scale, gain=got.gain, ids=got.ids)
    hop_r, hop_a, hop_b = {0: hop(got.send_r, [(0, 1)])}, {}, {}
    small2 = hop(got.small, swap)
    pair = dict(small=got.small, small2=small2, w=w, w2=w2)
    for t in range(1, STEPS):
        ins, outs = dict(stats0=got.stats), dict(sums)
        if t < RELAY_END:
            ins |= relay
        if t < CHUNKS:
            ins |= dict(hidden=hidden_in)
            outs |= dict(send_r=full)
        if t in A_HOPS:
            ins |= dict(recv_r=hop_r[t - 2])
            outs |= dict(send_a=half)
        if t >= 2:
            outs |= dict(send_b=half)
        if t >= PAIR_START:
            ins |= pair | dict(recv_b=hop_b[t - 2])
            if t - 2 in A_HOPS:
                ins |= dict(recv_a=hop_a[t - 2])
        if t == STEPS - 1:
            outs = dict(send_b=half, table=((2 * 32, 128), jnp.float32))
        got = run_step(t, ins, outs)
        if t in B_HOPS:
            hop_b[t] = hop(got.send_b, hop_pairs(t))
        if t in A_HOPS:
            hop_a[t] = hop(got.send_a, [(1, 2)])
        if t in R_HOPS:
            hop_r[t] = hop(got.send_r, [(0, 1)])
    arrived = lax.all_to_all(got.table, (C, Z, Y), 0, 0, tiled=True)
    ins = dict(arrived=arrived, part0=hop_b[8], part1=hop_b[9], part2=hop_b[10], last=got.send_b)
    outs = dict(out=half, balance=((1,), jnp.float32))
    token_total = float(batches * rows * lax.axis_size(Z) * lax.axis_size(Y))
    kernel = functools.partial(final_kernel, token_total)
    scratch = dict(sem=pltpu.SemaphoreType.DMA)
    got = call(kernel, ins, outs, scratch, (), [pltpu.HBM, pltpu.SMEM])
    return got.out[None], got.balance


def solution(mesh):
    torus = Mesh(mesh.devices.reshape(CHIPS, 2, 8, 4), (X, C, Z, Y))
    dp = (Z, Y)

    return jax.shard_map(
        per_device,
        mesh=torus,
        in_specs=(
            P(None, dp, None),
            P(SEC, None),
            P(SEC, None, None),
            P(SEC, None, None),
            P(SEC, None, None),
            P(SEC, None, dp, None),
        ),
        out_specs=(P(SEC, dp, None), P(SEC)),
        check_vma=False,
    )
```

```python
import functools
from types import SimpleNamespace

import jax
import jax.numpy as jnp
from jax import lax
from jax.experimental import pallas as pl
from jax.experimental.pallas import tpu as pltpu
from jax.sharding import Mesh
from jax.sharding import PartitionSpec as P


X, C, Z, Y = "xczy"
SEC = (X, C)
CHIPS = 4
CHUNKS = 4
RELAY_END = 6
PAIR_START = 4
STEPS = 13
COLS = 256
WIDE = 512
VMEM_LIMIT = 12 * 1024 * 1024


def front(rows, load_x, load_gain, load_router, load_scale, ids, r):
    width = r.nrm.shape[1]
    acc = None
    for c in range(0, width, COLS):
        xs = load_x(c, COLS).astype(jnp.float32)
        acc = xs * xs if acc is None else acc + xs * xs
    mean_square = jnp.sum(acc, axis=-1, keepdims=True) * jnp.float32(1.0 / width)
    inv = lax.rsqrt(mean_square + 1e-06)
    for c in range(0, width, COLS):
        xs = load_x(c, COLS).astype(jnp.float32)
        normed = xs * inv * load_gain(c, COLS).astype(jnp.float32)
        r.nrm[0:rows, c : c + COLS] = normed
        r.nbf[0:rows, c : c + COLS] = normed.astype(jnp.bfloat16)
    logits = lax.dot_general(
        r.nbf[0:rows, :],
        load_router(),
        (((1,), (1,)), ((), ())),
        preferred_element_type=jnp.float32,
    )
    picks = ids.shape[0]
    named = jnp.concatenate([ids.astype(jnp.float32), jnp.zeros((8 - picks, rows))], axis=0)
    named = jnp.transpose(named).astype(jnp.int32)

    def hits(shape, first):
        expert = lax.broadcasted_iota(jnp.int32, shape, 1) - first
        hit = named[:, 0:1] == expert
        for k in range(1, picks):
            hit = hit | (named[:, k : k + 1] == expert)
        return jnp.where(hit, 1.0, 0.0).astype(jnp.float32)

    exponent = jnp.exp(logits)
    probs = exponent / jnp.sum(exponent, axis=1, keepdims=True)
    gates = (probs * hits(probs.shape, 0)).astype(jnp.bfloat16)
    for c in range(0, width, COLS):
        channel = jnp.dot(gates, load_scale(c, COLS), preferred_element_type=jnp.float32)
        r.mixed[0:rows, c : c + COLS] = (r.nrm[0:rows, c : c + COLS] * channel).astype(
            jnp.bfloat16
        )
    return (
        jnp.sum(probs, axis=0, keepdims=True),
        jnp.sum(hits((rows, 128), 64), axis=0, keepdims=True),
    )


def add_update(rows, cur, n, update):
    cur[0:rows, n : n + WIDE] = (cur[0:rows, n : n + WIDE].astype(jnp.float32) + update).astype(
        jnp.bfloat16
    )


def mix_block(rows, cur, mixed, w, n):
    weight = w[:, n : n + WIDE]
    update = jnp.dot(mixed[0:rows, :], weight, preferred_element_type=jnp.float32)
    add_update(rows, cur, n, update)


def mix_all(rows, cur, mixed, load_w):
    width = cur.shape[1]
    blocks = range(0, width, WIDE)
    sums = {n: None for n in blocks}
    for k in range(0, width, COLS):
        for n in blocks:
            part = jnp.dot(
                mixed[0:rows, k : k + COLS],
                load_w(slice(k, k + COLS), slice(n, n + WIDE)),
                preferred_element_type=jnp.float32,
            )
            sums[n] = part if k == 0 else sums[n] + part
    for n in blocks:
        add_update(rows, cur, n, sums[n])


def add_stats(stats, layer, sums, counts):
    stats[pl.ds(layer, 1), :] += counts
    stats[pl.ds(layer, 1), 0 : sums.shape[1]] += sums


def relay_layer(r, cur, chunk, weight, waits=None):
    rows = cur.shape[0]
    sums, counts = front(
        rows,
        lambda c, n: cur[0:rows, c : c + n],
        lambda c, n: r.gain[:, c : c + n],
        lambda: r.router[...],
        lambda c, n: r.scale[:, c : c + n],
        jnp.concatenate([r.ids[2 * chunk], r.ids[2 * chunk + 1]], axis=1),
        r,
    )
    if waits is None:
        mix_all(rows, cur, r.mixed, lambda k, n: weight[k, n])
        return sums, counts
    for i, n in enumerate(range(0, cur.shape[1], WIDE)):
        waits[i].wait()
        mix_block(rows, cur, r.mixed, weight, n)
    return sums, counts


def column_copies(source, to, sems):
    return [
        pltpu.make_async_copy(source.at[:, pl.ds(n, WIDE)], to.at[:, pl.ds(n, WIDE)], sems.at[i])
        for i, n in enumerate(range(0, to.shape[1], WIDE))
    ]


def run_all(copies):
    for copy in copies:
        copy.start()
    for copy in copies:
        copy.wait()


def hidden_copies(r, chunk, to):
    return [
        pltpu.make_async_copy(r.hidden.at[2 * chunk + b], to.at[pl.ds(64 * b, 64)], r.xsem.at[b])
        for b in range(2)
    ]


def first_step(r, first, second):
    pairs = ((r.gain0, r.gain), (r.ids0, r.ids), (r.router0, r.router), (r.scale0, r.scale))
    small = [pltpu.make_async_copy(a, b, r.ssem.at[i]) for i, (a, b) in enumerate(pairs)]
    weight = column_copies(r.w0, r.wr, r.wsem)
    for copy in small:
        copy.start()

    @pl.when(first)
    def _():
        for copy in hidden_copies(r, 0, r.send_r):
            copy.start()

    @pl.when(first | second)
    def _():
        for copy in weight[:2]:
            copy.start()

    for copy in small:
        copy.wait()

    @pl.when(first)
    def _():
        for copy in hidden_copies(r, 0, r.send_r):
            copy.wait()

    @pl.when(first | second)
    def _():
        for copy in weight[2:]:
            copy.start()

    @pl.when(first)
    def _():
        sums, counts = relay_layer(r, r.send_r, 0, r.wr, weight)
        add_stats(r.stats, 0, sums, counts)

    @pl.when(second)
    def _():
        for copy in weight:
            copy.wait()

    @pl.when(jnp.logical_not(first | second))
    def _():
        ids = jnp.concatenate([r.ids[m] for m in range(r.ids.shape[0])], axis=0)
        r.small[0:60, :] = r.router[...]
        r.small[64:124, :] = r.scale[...]
        r.small[128:129, :] = r.gain[...]
        r.small[144:176, 0:64] = ids.astype(jnp.float32).astype(jnp.bfloat16)


def relay_step(t, r, first, second, core):
    cur = r.cur if t >= 2 else r.send_r
    if t < CHUNKS:

        @pl.when(first)
        def _():
            run_all(hidden_copies(r, t, cur))

    if t >= 2:

        @pl.when(second)
        def _():
            cur[...] = r.recv_r[...]

    @pl.when(first if t < 2 else (second if t >= CHUNKS else first | second))
    def _():
        sums, counts = relay_layer(r, cur, t - 2 * core, r.wr)
        add_stats(r.stats, core, sums, counts)

    if 2 <= t < CHUNKS:

        @pl.when(first)
        def _():
            r.send_r[...] = cur[...]

    if t >= 2:

        @pl.when(second)
        def _():
            r.send_a[...] = cur[0:64, :]
            r.send_b[...] = cur[64:128, :]


def pair_step(t, r, chip, core):
    late = jnp.where(chip == 2, core, 1 - core)
    chunk = t - 2 - 2 * chip - late
    cur = r.send_b

    @pl.when((chip >= 1) & (chunk >= 0) & (chunk < CHUNKS))
    def _():
        if hasattr(r, "recv_a"):
            from_a = (chip == 1) & (core == 0)

            @pl.when(from_a)
            def _():
                cur[...] = r.recv_a[...]

            @pl.when(jnp.logical_not(from_a))
            def _():
                cur[...] = r.recv_b[...]
        else:
            cur[...] = r.recv_b[...]
        batch = 2 * chunk + 1 - late

        def one(layer, carry):
            own = layer == core

            def pick(rows, c, n):
                return jnp.where(own, r.small[rows, c : c + n], r.small2[rows, c : c + n])

            table = pick(slice(144, 176), 0, 64).astype(jnp.float32)
            ids = table[0:4]
            for m in range(1, 8):
                ids = jnp.where(batch == m, table[4 * m : 4 * m + 4], ids)
            sums, counts = front(
                64,
                lambda c, n: cur[:, c : c + n],
                lambda c, n: pick(slice(128, 129), c, n),
                lambda: pick(slice(0, 60), 0, cur.shape[1]),
                lambda c, n: pick(slice(64, 124), c, n),
                ids.astype(jnp.int32),
                r,
            )

            mix_all(64, cur, r.mixed, lambda k, n: jnp.where(own, r.w[k, n], r.w2[k, n]))
            add_stats(r.stats, layer, sums, counts)
            return carry

        lax.fori_loop(0, 2, one, 0)


def step_kernel(t, names, *refs):
    r = SimpleNamespace(**dict(zip(names, refs)))
    chip, core = lax.axis_index(X), lax.axis_index(C)
    first, second = (chip == 0) & (core == 0), (chip == 0) & (core == 1)
    if t:
        r.stats[...] = r.stats0[...]
    else:
        r.stats[...] = jnp.zeros_like(r.stats)
        first_step(r, first, second)
    if 0 < t < RELAY_END:
        relay_step(t, r, first, second, core)
    if t >= PAIR_START:
        pair_step(t, r, chip, core)
    if t == STEPS - 1:
        for layer in range(2):
            row = r.stats[layer : layer + 1, :]
            r.table[32 * layer : 32 * layer + 32, :] = jnp.broadcast_to(row, (32, 128))


def final_kernel(token_total, arrived, p0, p1, p2, p3, odd, even, out, balance, sem):
    chip, core = lax.axis_index(X), lax.axis_index(C)
    for own, parts in ((1, (p0, p1, p2, odd)), (0, (p1, p2, p3, even))):
        for k, part in enumerate(parts):

            @pl.when((chip == k) & (core == own))
            def _():
                pltpu.make_async_copy(part, out, sem).start()

    total = jnp.sum(arrived[...], axis=0, keepdims=True)
    counts = pltpu.roll(total, 64, 1)
    at = lax.broadcasted_iota(jnp.int32, total.shape, 1)
    terms = jnp.where(at < 60, (counts / (token_total * 4.0)) * (total / token_total), 0.0)
    balance[0] = 60.0 * jnp.sum(terms)
    pltpu.make_async_copy(even, out, sem).wait()


def call(kernel, ins, outs, scratch, hbm=(), places=None):
    spaces = [pltpu.HBM if n in hbm else pltpu.VMEM for n in ins]
    args = [pltpu.with_memory_space_constraint(v, m) for v, m in zip(ins.values(), spaces)]
    places = places or [pltpu.VMEM] * len(outs)
    got = pl.pallas_call(
        kernel,
        out_shape=[place(*v) for place, v in zip(places, outs.values())],
        in_specs=[pl.BlockSpec(memory_space=m) for m in spaces],
        out_specs=[pl.BlockSpec(memory_space=place) for place in places],
        scratch_shapes=list(scratch.values()),
        compiler_params=pltpu.CompilerParams(vmem_limit_bytes=VMEM_LIMIT),
        cost_estimate=pl.CostEstimate(
            flops=2 * 64 * 2048 * 2048 * 2, bytes_accessed=8 * 1024 * 1024, transcendentals=0
        ),
    )(*args)
    return SimpleNamespace(**dict(zip(outs, got)))


R_HOPS = range(CHUNKS)
A_HOPS = range(2, RELAY_END)
B_HOPS = range(2, STEPS - 1)


def run_step(t, ins, outs):
    rows = 128 if t < RELAY_END else 64
    scratch = dict(
        nrm=pltpu.VMEM((rows, 2048), jnp.float32), nbf=pltpu.VMEM((rows, 2048), jnp.bfloat16)
    )
    scratch |= dict(mixed=pltpu.VMEM((rows, 2048), jnp.bfloat16))
    if t == STEPS - 1:
        scratch |= dict(stats=pltpu.VMEM((8, 128), jnp.float32))
    if 2 <= t < RELAY_END:
        scratch |= dict(cur=pltpu.VMEM((128, 2048), jnp.bfloat16))
    if t < CHUNKS:
        scratch |= dict(xsem=pltpu.SemaphoreType.DMA((2,)))
    if t == 0:
        scratch |= dict(wsem=pltpu.SemaphoreType.DMA((4,)), ssem=pltpu.SemaphoreType.DMA((4,)))
    kernel = functools.partial(step_kernel, t, (*ins, *outs, *scratch))
    hbm = tuple(dict(hidden=0, w0=0, router0=0, scale0=0, gain0=0, ids0=0))
    return call(kernel, ins, outs, scratch, hbm)


def hop_pairs(t):
    pairs = [(1, 3)] if t in A_HOPS else []
    for chip in (1, 2, 3):
        for core in range(2):
            late = core if chip == 2 else 1 - core
            chunk = t - 2 - 2 * chip - late
            if 0 <= chunk < CHUNKS and chip < CHIPS - 1:
                pairs.append((2 * chip + core, 2 * (chip + 1) + 1 - core))
            if 0 <= chunk < CHUNKS - 1 and chip == CHIPS - 1:
                pairs.append((2 * chip + core, 2 * chunk + core))
    return pairs


def per_device(hidden_in, norm_gain, router_weight, expert_scale, mix_weight, routes):
    batches, rows, width = hidden_in.shape
    router = jnp.transpose(router_weight[0])
    ids = jnp.transpose(routes[0], (0, 2, 1))
    scale, w = expert_scale[0], mix_weight[0]
    swap = [(2 * x + c, 2 * x + 1 - c) for x in range(1, CHIPS) for c in range(2)]

    def hop(x, pairs):
        return lax.ppermute(x, SEC, pairs)

    half = ((rows, width), jnp.bfloat16)
    full = ((2 * rows, width), jnp.bfloat16)
    sums = dict(stats=((8, 128), jnp.float32))

    def like(x):
        return (x.shape, x.dtype)

    w2 = hop(w, swap)
    got = run_step(
        0,
        dict(hidden=hidden_in, w0=w, router0=router, scale0=scale, gain0=norm_gain, ids0=ids),
        dict(
            wr=like(w),
            router=like(router),
            scale=like(scale),
            gain=like(norm_gain),
            ids=like(ids),
            send_r=full,
            small=((176, width), jnp.bfloat16),
        )
        | sums,
    )
    relay = dict(wr=got.wr, router=got.router, scale=got.scale, gain=got.gain, ids=got.ids)
    hop_r, hop_a, hop_b = {0: hop(got.send_r, [(0, 1)])}, {}, {}
    small2 = hop(got.small, swap)
    pair = dict(small=got.small, small2=small2, w=w, w2=w2)
    for t in range(1, STEPS):
        ins, outs = dict(stats0=got.stats), dict(sums)
        if t < RELAY_END:
            ins |= relay
        if t < CHUNKS:
            ins |= dict(hidden=hidden_in)
            outs |= dict(send_r=full)
        if t in A_HOPS:
            ins |= dict(recv_r=hop_r[t - 2])
            outs |= dict(send_a=half)
        if t >= 2:
            outs |= dict(send_b=half)
        if t >= PAIR_START:
            ins |= pair | dict(recv_b=hop_b[t - 2])
            if t - 3 in A_HOPS:
                ins |= dict(recv_a=hop_a[t - 3])
        if t == STEPS - 1:
            outs = dict(send_b=half, table=((2 * 32, 128), jnp.float32))
        got, before = run_step(t, ins, outs), got
        if t in B_HOPS:
            hop_b[t] = hop(got.send_b, hop_pairs(t))
        if t in A_HOPS:
            hop_a[t] = hop(got.send_a, [(1, 2)])
        if t in R_HOPS:
            hop_r[t] = hop(got.send_r, [(0, 1)])
    arrived = lax.all_to_all(got.table, (C, Z, Y), 0, 0, tiled=True)
    ins = dict(arrived=arrived, p0=hop_b[8], p1=hop_b[9], p2=hop_b[10], p3=hop_b[11])
    ins |= dict(odd=before.send_b, even=got.send_b)
    outs = dict(out=half, balance=((1,), jnp.float32))
    token_total = float(batches * rows * lax.axis_size(Z) * lax.axis_size(Y))
    kernel = functools.partial(final_kernel, token_total)
    scratch = dict(sem=pltpu.SemaphoreType.DMA)
    got = call(kernel, ins, outs, scratch, (), [pltpu.HBM, pltpu.SMEM])
    return got.out[None], got.balance


def solution(mesh):
    torus = Mesh(mesh.devices.reshape(CHIPS, 2, 8, 4), (X, C, Z, Y))
    dp = (Z, Y)

    return jax.shard_map(
        per_device,
        mesh=torus,
        in_specs=(
            P(None, dp, None),
            P(SEC, None),
            P(SEC, None, None),
            P(SEC, None, None),
            P(SEC, None, None),
            P(SEC, None, dp, None),
        ),
        out_specs=(P(SEC, dp, None), P(SEC)),
        check_vma=False,
    )
```

```python
import functools
from types import SimpleNamespace

import jax
import jax.numpy as jnp
from jax import lax
from jax.experimental import pallas as pl
from jax.experimental.pallas import tpu as pltpu
from jax.sharding import Mesh
from jax.sharding import PartitionSpec as P


X, C, Z, Y = "xczy"
SEC = (X, C)
CHIPS = 4
CHUNKS = 4
RELAY_END = 6
PAIR_START = 4
STEPS = 12
COLS = 256
WIDE = 512
VMEM_LIMIT = 12 * 1024 * 1024


def front(rows, load_x, load_gain, load_router, load_scale, ids, r):
    width = r.nrm.shape[1]
    acc = None
    for c in range(0, width, COLS):
        xs = load_x(c, COLS).astype(jnp.float32)
        acc = xs * xs if acc is None else acc + xs * xs
    mean_square = jnp.sum(acc, axis=-1, keepdims=True) * jnp.float32(1.0 / width)
    inv = lax.rsqrt(mean_square + 1e-06)
    for c in range(0, width, COLS):
        xs = load_x(c, COLS).astype(jnp.float32)
        normed = xs * inv * load_gain(c, COLS).astype(jnp.float32)
        r.nrm[0:rows, c : c + COLS] = normed
        r.nbf[0:rows, c : c + COLS] = normed.astype(jnp.bfloat16)
    logits = lax.dot_general(
        r.nbf[0:rows, :],
        load_router(),
        (((1,), (1,)), ((), ())),
        preferred_element_type=jnp.float32,
    )
    picks = ids.shape[0]
    named = jnp.concatenate([ids.astype(jnp.float32), jnp.zeros((8 - picks, rows))], axis=0)
    named = jnp.transpose(named).astype(jnp.int32)

    def hits(shape, first):
        expert = lax.broadcasted_iota(jnp.int32, shape, 1) - first
        hit = named[:, 0:1] == expert
        for k in range(1, picks):
            hit = hit | (named[:, k : k + 1] == expert)
        return jnp.where(hit, 1.0, 0.0).astype(jnp.float32)

    exponent = jnp.exp(logits)
    probs = exponent / jnp.sum(exponent, axis=1, keepdims=True)
    gates = (probs * hits(probs.shape, 0)).astype(jnp.bfloat16)
    for c in range(0, width, COLS):
        channel = jnp.dot(gates, load_scale(c, COLS), preferred_element_type=jnp.float32)
        r.mixed[0:rows, c : c + COLS] = (r.nrm[0:rows, c : c + COLS] * channel).astype(
            jnp.bfloat16
        )
    return (
        jnp.sum(probs, axis=0, keepdims=True),
        jnp.sum(hits((rows, 128), 64), axis=0, keepdims=True),
    )


def add_update(rows, cur, n, update):
    cur[0:rows, n : n + WIDE] = (cur[0:rows, n : n + WIDE].astype(jnp.float32) + update).astype(
        jnp.bfloat16
    )


def mix_block(rows, cur, mixed, w, n):
    weight = w[:, n : n + WIDE]
    update = jnp.dot(mixed[0:rows, :], weight, preferred_element_type=jnp.float32)
    add_update(rows, cur, n, update)


def mix_all(rows, cur, mixed, load_w):
    width = cur.shape[1]
    blocks = range(0, width, WIDE)
    sums = {n: None for n in blocks}
    for k in range(0, width, COLS):
        for n in blocks:
            part = jnp.dot(
                mixed[0:rows, k : k + COLS],
                load_w(slice(k, k + COLS), slice(n, n + WIDE)),
                preferred_element_type=jnp.float32,
            )
            sums[n] = part if k == 0 else sums[n] + part
    for n in blocks:
        add_update(rows, cur, n, sums[n])


def add_stats(stats, layer, sums, counts):
    stats[pl.ds(layer, 1), :] += counts
    stats[pl.ds(layer, 1), 0 : sums.shape[1]] += sums


def relay_layer(r, cur, chunk, weight, waits=None):
    rows = cur.shape[0]
    sums, counts = front(
        rows,
        lambda c, n: cur[0:rows, c : c + n],
        lambda c, n: r.gain[:, c : c + n],
        lambda: r.router[...],
        lambda c, n: r.scale[:, c : c + n],
        jnp.concatenate([r.ids[2 * chunk], r.ids[2 * chunk + 1]], axis=1),
        r,
    )
    if waits is None:
        mix_all(rows, cur, r.mixed, lambda k, n: weight[k, n])
        return sums, counts
    for i, n in enumerate(range(0, cur.shape[1], WIDE)):
        waits[i].wait()
        mix_block(rows, cur, r.mixed, weight, n)
    return sums, counts


def column_copies(source, to, sems):
    return [
        pltpu.make_async_copy(source.at[:, pl.ds(n, WIDE)], to.at[:, pl.ds(n, WIDE)], sems.at[i])
        for i, n in enumerate(range(0, to.shape[1], WIDE))
    ]


def run_all(copies):
    for copy in copies:
        copy.start()
    for copy in copies:
        copy.wait()


def hidden_copies(r, chunk, to):
    return [
        pltpu.make_async_copy(r.hidden.at[2 * chunk + b], to.at[pl.ds(64 * b, 64)], r.xsem.at[b])
        for b in range(2)
    ]


def first_step(r, first, second):
    pairs = ((r.gain0, r.gain), (r.ids0, r.ids), (r.router0, r.router), (r.scale0, r.scale))
    small = [pltpu.make_async_copy(a, b, r.ssem.at[i]) for i, (a, b) in enumerate(pairs)]
    weight = column_copies(r.w0, r.wr, r.wsem)
    for copy in small:
        copy.start()

    @pl.when(first)
    def _():
        for copy in hidden_copies(r, 0, r.send_r):
            copy.start()

    @pl.when(first | second)
    def _():
        for copy in weight[:2]:
            copy.start()

    for copy in small:
        copy.wait()

    @pl.when(first)
    def _():
        for copy in hidden_copies(r, 0, r.send_r):
            copy.wait()

    @pl.when(first | second)
    def _():
        for copy in weight[2:]:
            copy.start()

    @pl.when(first)
    def _():
        sums, counts = relay_layer(r, r.send_r, 0, r.wr, weight)
        add_stats(r.stats, 0, sums, counts)

    @pl.when(second)
    def _():
        for copy in weight:
            copy.wait()

    @pl.when(jnp.logical_not(first | second))
    def _():
        ids = jnp.concatenate([r.ids[m] for m in range(r.ids.shape[0])], axis=0)
        r.small[0:60, :] = r.router[...]
        r.small[64:124, :] = r.scale[...]
        r.small[128:129, :] = r.gain[...]
        r.small[144:176, 0:64] = ids.astype(jnp.float32).astype(jnp.bfloat16)


def relay_step(t, r, first, second, core):
    cur = r.cur if t >= 2 else r.send_r
    if t < CHUNKS:

        @pl.when(first)
        def _():
            run_all(hidden_copies(r, t, cur))

    if t >= 2:

        @pl.when(second)
        def _():
            cur[...] = r.recv_r[...]

    @pl.when(first if t < 2 else (second if t >= CHUNKS else first | second))
    def _():
        sums, counts = relay_layer(r, cur, t - 2 * core, r.wr)
        add_stats(r.stats, core, sums, counts)

    if 2 <= t < CHUNKS:

        @pl.when(first)
        def _():
            r.send_r[...] = cur[...]

    if t >= 2:

        @pl.when(second)
        def _():
            r.send_b[...] = cur[0:64, :]
            r.send_a[...] = cur[64:128, :]


def pair_step(t, r, chip, core):
    chunk = t - 2 - 2 * chip
    cur = r.send_b

    @pl.when((chip >= 1) & (chunk >= 0) & (chunk < CHUNKS))
    def _():
        if hasattr(r, "recv_a"):
            from_a = (chip == 1) & (core == 0)

            @pl.when(from_a)
            def _():
                cur[...] = r.recv_a[...]

            @pl.when(jnp.logical_not(from_a))
            def _():
                cur[...] = r.recv_b[...]
        else:
            cur[...] = r.recv_b[...]
        batch = 2 * chunk + jnp.where(chip == 1, 1 - core, core)

        def one(layer, carry):
            own = layer == core

            def pick(rows, c, n):
                return jnp.where(own, r.small[rows, c : c + n], r.small2[rows, c : c + n])

            table = pick(slice(144, 176), 0, 64).astype(jnp.float32)
            ids = table[0:4]
            for m in range(1, 8):
                ids = jnp.where(batch == m, table[4 * m : 4 * m + 4], ids)
            sums, counts = front(
                64,
                lambda c, n: cur[:, c : c + n],
                lambda c, n: pick(slice(128, 129), c, n),
                lambda: pick(slice(0, 60), 0, cur.shape[1]),
                lambda c, n: pick(slice(64, 124), c, n),
                ids.astype(jnp.int32),
                r,
            )

            mix_all(64, cur, r.mixed, lambda k, n: jnp.where(own, r.w[k, n], r.w2[k, n]))
            add_stats(r.stats, layer, sums, counts)
            return carry

        lax.fori_loop(0, 2, one, 0)


def step_kernel(t, names, *refs):
    r = SimpleNamespace(**dict(zip(names, refs)))
    chip, core = lax.axis_index(X), lax.axis_index(C)
    first, second = (chip == 0) & (core == 0), (chip == 0) & (core == 1)
    if t:
        r.stats[...] = r.stats0[...]
    else:
        r.stats[...] = jnp.zeros_like(r.stats)
        first_step(r, first, second)
    if 0 < t < RELAY_END:
        relay_step(t, r, first, second, core)
    if t >= PAIR_START:
        pair_step(t, r, chip, core)
    if t == STEPS - 1:
        for layer in range(2):
            row = r.stats[layer : layer + 1, :]
            r.table[32 * layer : 32 * layer + 32, :] = jnp.broadcast_to(row, (32, 128))


def final_kernel(token_total, arrived, part0, part1, part2, last, out, balance, sem):
    chip = lax.axis_index(X)
    for k, part in enumerate((part0, part1, part2, last)):

        @pl.when(chip == k)
        def _():
            pltpu.make_async_copy(part, out, sem).start()

    total = jnp.sum(arrived[...], axis=0, keepdims=True)
    counts = pltpu.roll(total, 64, 1)
    at = lax.broadcasted_iota(jnp.int32, total.shape, 1)
    terms = jnp.where(at < 60, (counts / (token_total * 4.0)) * (total / token_total), 0.0)
    balance[0] = 60.0 * jnp.sum(terms)
    pltpu.make_async_copy(last, out, sem).wait()


def call(kernel, ins, outs, scratch, hbm=(), places=None):
    spaces = [pltpu.HBM if n in hbm else pltpu.VMEM for n in ins]
    args = [pltpu.with_memory_space_constraint(v, m) for v, m in zip(ins.values(), spaces)]
    places = places or [pltpu.VMEM] * len(outs)
    got = pl.pallas_call(
        kernel,
        out_shape=[place(*v) for place, v in zip(places, outs.values())],
        in_specs=[pl.BlockSpec(memory_space=m) for m in spaces],
        out_specs=[pl.BlockSpec(memory_space=place) for place in places],
        scratch_shapes=list(scratch.values()),
        compiler_params=pltpu.CompilerParams(vmem_limit_bytes=VMEM_LIMIT),
        cost_estimate=pl.CostEstimate(
            flops=2 * 64 * 2048 * 2048 * 2, bytes_accessed=8 * 1024 * 1024, transcendentals=0
        ),
    )(*args)
    return SimpleNamespace(**dict(zip(outs, got)))


R_HOPS = range(CHUNKS)
A_HOPS = range(2, RELAY_END)
B_HOPS = range(2, STEPS - 1)


def run_step(t, ins, outs):
    rows = 128 if t < RELAY_END else 64
    scratch = dict(
        nrm=pltpu.VMEM((rows, 2048), jnp.float32), nbf=pltpu.VMEM((rows, 2048), jnp.bfloat16)
    )
    scratch |= dict(mixed=pltpu.VMEM((rows, 2048), jnp.bfloat16))
    if t == STEPS - 1:
        scratch |= dict(stats=pltpu.VMEM((8, 128), jnp.float32))
    if 2 <= t < RELAY_END:
        scratch |= dict(cur=pltpu.VMEM((128, 2048), jnp.bfloat16))
    if t < CHUNKS:
        scratch |= dict(xsem=pltpu.SemaphoreType.DMA((2,)))
    if t == 0:
        scratch |= dict(wsem=pltpu.SemaphoreType.DMA((4,)), ssem=pltpu.SemaphoreType.DMA((4,)))
    kernel = functools.partial(step_kernel, t, (*ins, *outs, *scratch))
    hbm = tuple(dict(hidden=0, w0=0, router0=0, scale0=0, gain0=0, ids0=0))
    return call(kernel, ins, outs, scratch, hbm)


def hop_pairs(t):
    pairs = [(1, 3)] if t in A_HOPS else []
    for chip in (1, 2, 3):
        chunk = t - 2 - 2 * chip
        if 0 <= chunk < CHUNKS:
            if chip < CHIPS - 1:
                swap = int(chip == 1)
                pairs += [(2 * chip + c, 2 * (chip + 1) + (c ^ swap)) for c in range(2)]
            else:
                pairs += [(2 * chip + c, 2 * chunk + c) for c in range(2)]
    return pairs


def per_device(hidden_in, norm_gain, router_weight, expert_scale, mix_weight, routes):
    batches, rows, width = hidden_in.shape
    router = jnp.transpose(router_weight[0])
    ids = jnp.transpose(routes[0], (0, 2, 1))
    scale, w = expert_scale[0], mix_weight[0]
    swap = [(2 * x + c, 2 * x + 1 - c) for x in range(1, CHIPS) for c in range(2)]

    def hop(x, pairs):
        return lax.ppermute(x, SEC, pairs)

    half = ((rows, width), jnp.bfloat16)
    full = ((2 * rows, width), jnp.bfloat16)
    sums = dict(stats=((8, 128), jnp.float32))

    def like(x):
        return (x.shape, x.dtype)

    w2 = hop(w, swap)
    got = run_step(
        0,
        dict(hidden=hidden_in, w0=w, router0=router, scale0=scale, gain0=norm_gain, ids0=ids),
        dict(
            wr=like(w),
            router=like(router),
            scale=like(scale),
            gain=like(norm_gain),
            ids=like(ids),
            send_r=full,
            small=((176, width), jnp.bfloat16),
        )
        | sums,
    )
    relay = dict(wr=got.wr, router=got.router, scale=got.scale, gain=got.gain, ids=got.ids)
    hop_r, hop_a, hop_b = {0: hop(got.send_r, [(0, 1)])}, {}, {}
    small2 = hop(got.small, swap)
    pair = dict(small=got.small, small2=small2, w=w, w2=w2)
    for t in range(1, STEPS):
        ins, outs = dict(stats0=got.stats), dict(sums)
        if t < RELAY_END:
            ins |= relay
        if t < CHUNKS:
            ins |= dict(hidden=hidden_in)
            outs |= dict(send_r=full)
        if t in A_HOPS:
            ins |= dict(recv_r=hop_r[t - 2])
            outs |= dict(send_a=half)
        if t >= 2:
            outs |= dict(send_b=half)
        if t >= PAIR_START:
            ins |= pair | dict(recv_b=hop_b[t - 2])
            if t - 2 in A_HOPS:
                ins |= dict(recv_a=hop_a[t - 2])
        if t == STEPS - 1:
            outs = dict(send_b=half, table=((2 * 32, 128), jnp.float32))
        got = run_step(t, ins, outs)
        if t in B_HOPS:
            hop_b[t] = hop(got.send_b, hop_pairs(t))
        if t in A_HOPS:
            hop_a[t] = hop(got.send_a, [(1, 2)])
        if t in R_HOPS:
            hop_r[t] = hop(got.send_r, [(0, 1)])
    arrived = lax.all_to_all(got.table, (C, Z, Y), 0, 0, tiled=True)
    ins = dict(arrived=arrived, part0=hop_b[8], part1=hop_b[9], part2=hop_b[10], last=got.send_b)
    outs = dict(out=half, balance=((1,), jnp.float32))
    token_total = float(batches * rows * lax.axis_size(Z) * lax.axis_size(Y))
    kernel = functools.partial(final_kernel, token_total)
    scratch = dict(sem=pltpu.SemaphoreType.DMA)
    got = call(kernel, ins, outs, scratch, (), [pltpu.HBM, pltpu.SMEM])
    return got.out[None], got.balance


def solution(mesh):
    torus = Mesh(mesh.devices.reshape(CHIPS, 2, 8, 4), (X, C, Z, Y))
    dp = (Z, Y)

    return jax.shard_map(
        per_device,
        mesh=torus,
        in_specs=(
            P(None, dp, None),
            P(SEC, None),
            P(SEC, None, None),
            P(SEC, None, None),
            P(SEC, None, None),
            P(SEC, None, dp, None),
        ),
        out_specs=(P(SEC, dp, None), P(SEC)),
        check_vma=False,
    )
```
